32 devices in a mesh: slab: 8 (over z, y), sub: 4 (over x, core).
Axes of the slice: x: 2, y: 2, z: 4, core: 2. Of those that a mesh axis runs over, the one named last changes fastest.
Arguments:
- orbitals: float32 [16, 96, 9216], P('slab', None, 'sub'), may hold values from -6 to 6
- external_potential: float32 [64, 12288], P('slab', 'sub'), may hold values from -6 to 6
- corners: int32 [16, 2], replicated, may hold values from 0 to 63, as said below
- pair_list: int32 [16, 2], P('slab'), may hold values from 0 to 15, as said below
- pair_count: int32 [8], P('slab'), may hold values from 1 to 2, as said below
Outputs:
- applied_orbitals: float32 [16, 96, 9216], P('slab', None, 'sub')
The draws below stay inside these ranges and needn't reach their ends.
Inputs may be any that keep to these rules, and one draw needn't show every extreme that they name: `corners`: column 0 is the box's first x plane: for orbital o it lies in the 32 planes that begin at plane 8 * (o // 2), taken mod 64. Column 1 is the box's first z column (0 to 32). `pair_list`: orbital o is held by slab device o // 2. Rows 2 * d to 2 * d + 1 are the slots of slab device d; in each row (i, j), i is one of device d's orbitals, and j differs from i and is one of device d's orbitals or of device (d + 1) mod 8's. Rows that are not live hold such pairs too. `pair_count`: some slab device has 2 live slots in every draw.
All inputs are finite; a program needn't handle non-finite values.
Results may differ from the reference program's by a relative error of at most 0.0003.
Values sent between devices are 32-bit elements; how exact they have to be, the bound alone decides.
No kernel may reach another device: no remote copies, remote signals or barrier semaphores. Data moves between devices by JAX's collectives and lax.ppermute only.
A program may use at most 64 MiB of HBM per device.

```python
import math
import jax
import jax.numpy as jnp
from jax import lax

B = 96
GZ = 128
SX = 8
ORB_DEV = 2
PAIR_MAX = 2
NORB = 16
GX = 64
SLOTS = 16
N_SLAB = 8


def draw_corners(key, part):
    key_first, key_third = jax.random.split(jax.random.fold_in(key, 11))
    owner_slab = jnp.arange(NORB, dtype=jnp.int32) // ORB_DEV
    jitter = jax.random.randint(key_first, (NORB,), 0, 4 * SX, dtype=jnp.int32)
    first_plane = (owner_slab * SX + jitter) % GX
    third_plane = jax.random.randint(key_third, (NORB,), 0, GZ - B + 1, dtype=jnp.int32)
    return jnp.stack([first_plane, third_plane], axis=1)


def draw_pair_list(key, part):
    key_first, key_stride = jax.random.split(jax.random.fold_in(key, 37))
    owner_slab = jnp.arange(SLOTS, dtype=jnp.int32) // PAIR_MAX
    first_local = jax.random.randint(key_first, (SLOTS,), 0, ORB_DEV, dtype=jnp.int32)
    stride = jax.random.randint(key_stride, (SLOTS,), 1, 2 * ORB_DEV, dtype=jnp.int32)
    second_local = (first_local + stride) % (2 * ORB_DEV)
    first_orbital = owner_slab * ORB_DEV + first_local
    second_orbital = (owner_slab * ORB_DEV + second_local) % NORB
    return jnp.stack([first_orbital, second_orbital], axis=1)


def draw_pair_count(key, part):
    key_busy, key_light, key_top = jax.random.split(jax.random.fold_in(key, 23), 3)
    busy_slab = jax.random.randint(key_busy, (N_SLAB,), 0, 3, dtype=jnp.int32) == 0
    lighter = jax.random.randint(key_light, (N_SLAB,), 1, PAIR_MAX, dtype=jnp.int32)
    counts = jnp.where(busy_slab, PAIR_MAX, lighter).astype(jnp.int32)
    busiest = jax.random.randint(key_top, (), 0, N_SLAB, dtype=jnp.int32)
    return counts.at[busiest].set(PAIR_MAX)


def level_of(stream_key, extent, shards, low, high):
    loudness = 1.0
    for axis_at, shards_of in shards:
        steps = jax.random.uniform(jax.random.fold_in(jax.random.fold_in(stream_key, 6), axis_at), (shards_of,), jnp.float32, low / len(shards), high / len(shards))
        loudness = loudness * jnp.repeat(jnp.exp(steps), extent[axis_at] // shards_of).reshape((-1,) + (1,) * (len(extent) - 1 - axis_at))
    return loudness


def bell_draw(own_key, dims, deviation, bound, pieces=(), kind=jnp.bfloat16):
    drawn = deviation * jax.random.normal(own_key, dims, jnp.float32)
    if pieces:
        drawn = drawn * level_of(own_key, dims, pieces, -0.22, 0.18)
    return jnp.clip(drawn, -bound, bound).astype(kind)


def setup_inputs(seed: int = 0) -> dict:
    key_of = jax.random.split(jax.random.key(seed), 6)
    return {
        "orbitals": bell_draw(key_of[0], (NORB, B, B * B), 1.0, 6.0, ((0, 8), (2, 4)), jnp.float32),
        "external_potential": bell_draw(key_of[1], (GX, B * GZ), 1.0, 6.0, ((0, 8), (1, 4)), jnp.float32),
        "corners": draw_corners(jax.random.fold_in(key_of[5], 71), 0),
        "pair_list": draw_pair_list(jax.random.fold_in(key_of[5], 71), 0),
        "pair_count": draw_pair_count(jax.random.fold_in(key_of[5], 71), 0),
    }


SCREEN = 0.0008
FOCK_SHARE = 0.25
LOCAL_FACTOR = (3.0 / math.pi) ** (1.0 / 3.0)
EPSILON = 1e-06

def sine_table(box_edge):
    levels = jnp.arange(box_edge, dtype=jnp.int32).astype(jnp.float32) + 1.0
    factor = jnp.sqrt(jnp.asarray(2.0 / (box_edge + 1), jnp.float32))
    return factor * jnp.sin(math.pi * levels[:, None] * levels[None, :] / (box_edge + 1))

def sine_levels(box_edge):
    levels = jnp.arange(box_edge, dtype=jnp.int32).astype(jnp.float32) + 1.0
    return 2.0 - 2.0 * jnp.cos(math.pi * levels / (box_edge + 1))

def transform_all(volume, sine_matrix):
    volume = jnp.einsum('ax,xyz->ayz', sine_matrix, volume, precision=lax.Precision.HIGHEST)
    volume = jnp.einsum('by,xyz->xbz', sine_matrix, volume, precision=lax.Precision.HIGHEST)
    return jnp.einsum('cz,xyz->xyc', sine_matrix, volume, precision=lax.Precision.HIGHEST)

def solve_box(density):
    box_edge = density.shape[0]
    sine_matrix = sine_table(box_edge)
    levels = sine_levels(box_edge)
    kernel = 4.0 * math.pi / (levels[:, None, None] + levels[None, :, None] + levels[None, None, :] + SCREEN)
    return transform_all(kernel * transform_all(density, sine_matrix), sine_matrix)

def move_box(volume, shift_first, shift_third):
    box_edge = volume.shape[0]
    depth = volume.shape[2]
    first_source = jnp.arange(box_edge, dtype=jnp.int32) - shift_first.astype(jnp.int32)
    first_keep = ((first_source >= 0) & (first_source < box_edge)).astype(jnp.float32)
    volume = jnp.take(volume, jnp.clip(first_source, 0, box_edge - 1).astype(jnp.int32), axis=0) * first_keep[:, None, None]
    third_source = jnp.arange(depth, dtype=jnp.int32) - shift_third.astype(jnp.int32)
    third_keep = ((third_source >= 0) & (third_source < depth)).astype(jnp.float32)
    return jnp.take(volume, jnp.clip(third_source, 0, depth - 1).astype(jnp.int32), axis=2) * third_keep[None, None, :]

def pair_shifts(corner_first, corner_second, grid_planes):
    half_span = grid_planes // 2
    shift_first = (corner_second[0] - corner_first[0] + half_span) % grid_planes - half_span
    shift_third = corner_second[1] - corner_first[1]
    return (shift_first, shift_third)

def laplace_box(volume):
    padded = jnp.pad(volume, 1)
    beside_all = padded[2:, 1:-1, 1:-1] + padded[:-2, 1:-1, 1:-1]
    beside_all = beside_all + padded[1:-1, 2:, 1:-1] + padded[1:-1, :-2, 1:-1]
    beside_all = beside_all + padded[1:-1, 1:-1, 2:] + padded[1:-1, 1:-1, :-2]
    return beside_all - 6.0 * volume

def reference(orbitals, external_potential, corners, pair_list, pair_count):
    box_edge = orbitals.shape[1]
    boxes = orbitals.reshape(orbitals.shape[0], box_edge, box_edge, box_edge)
    grid_planes = external_potential.shape[0]
    grid_depth = external_potential.shape[1] // box_edge
    zero_index = jnp.zeros((), jnp.int32)
    offsets = jnp.arange(box_edge, dtype=jnp.int32)

    def deposit(density_grid, scan_item):
        volume, corner = scan_item
        placed = lax.dynamic_update_slice(jnp.zeros((box_edge, box_edge, grid_depth), jnp.float32), volume * volume, (zero_index, zero_index, corner[1].astype(jnp.int32)))
        planes = (corner[0] + offsets) % grid_planes
        return (density_grid.at[planes].add(placed.reshape(box_edge, box_edge * grid_depth)), None)
    density, _ = lax.scan(deposit, jnp.zeros((grid_planes, box_edge * grid_depth), jnp.float32), (boxes, corners))
    local_field = external_potential - LOCAL_FACTOR * jnp.cbrt(density + EPSILON)
    live_slots = (jnp.arange(PAIR_MAX, dtype=jnp.int32)[None, :] < pair_count[:, None]).astype(jnp.float32).reshape(-1)

    def one_pair(fock_terms, scan_item):
        pair_row, weight = scan_item
        first_orbital = pair_row[0]
        second_orbital = pair_row[1]
        shift_first, shift_third = pair_shifts(corners[first_orbital], corners[second_orbital], grid_planes)
        box_first = boxes[first_orbital]
        moved_box = move_box(boxes[second_orbital], shift_first, shift_third)
        potential = solve_box(box_first * moved_box)
        fock_terms = fock_terms.at[first_orbital].add(weight * potential * moved_box)
        fock_terms = fock_terms.at[second_orbital].add(weight * move_box(potential * box_first, -shift_first, -shift_third))
        return (fock_terms, None)
    exchange_field, _ = lax.scan(one_pair, jnp.zeros_like(boxes), (pair_list, live_slots))

    def finish(scan_item):
        volume, corner, exchange = scan_item
        planes = (corner[0] + offsets) % grid_planes
        taken = jnp.take(local_field, planes, axis=0).reshape(box_edge, box_edge, grid_depth)
        box_local = lax.dynamic_slice_in_dim(taken, corner[1].astype(jnp.int32), box_edge, 2)
        return -0.5 * laplace_box(volume) + box_local * volume - FOCK_SHARE * exchange
    result = lax.map(finish, (boxes, corners, exchange_field))
    return result.reshape(orbitals.shape)
```

```python
import functools
import math

import jax
import jax.numpy as jnp
import numpy as np
from jax import lax
from jax.experimental import pallas as pl
from jax.experimental.pallas import tpu as pltpu
from jax.sharding import PartitionSpec as P

REACH = 16
LANES = 128
GROUP = 8

SCREEN = 0.0008
FOCK_SHARE = 0.25
LOCAL_FACTOR = (3.0 / math.pi) ** (1.0 / 3.0)
EPSILON = 1e-06


def from_behind(value, axis, by):
    size = lax.axis_size(axis)
    return lax.ppermute(value, axis, [(i, (i + by) % size) for i in range(size)])


def partner(index, step, size):
    if size & (size - 1) == 0:
        return index ^ step
    return (size - index + step) % size


def exchange(pieces, axis):
    size = lax.axis_size(axis)
    received = []
    for step, piece in enumerate(pieces):
        pairs = [(i, partner(i, step, size)) for i in range(size)]
        if all(source == target for source, target in pairs):
            received.append(piece)
        else:
            received.append(lax.ppermute(piece, axis, pairs))
    return received


def split_bf16(value):
    high = value.astype(jnp.bfloat16)
    low = (value - high.astype(jnp.float32)).astype(jnp.bfloat16)
    return high, low


def sine_tables(box_edge):
    levels = np.arange(1, box_edge + 1, dtype=np.float64)
    sine = np.sqrt(2.0 / (box_edge + 1)) * np.sin(
        np.pi * levels[:, None] * levels[None, :] / (box_edge + 1)
    )
    sine = sine.astype(np.float32)
    high = sine.astype(jnp.bfloat16)
    low = (sine - high.astype(np.float32)).astype(jnp.bfloat16)
    padded = np.zeros((LANES, 2 * LANES), dtype=high.dtype)
    padded[:box_edge, :box_edge] = high
    padded[:box_edge, LANES : LANES + box_edge] = low
    stacked = np.concatenate([high, low], axis=0)
    return padded, stacked


def level_tables(box_edge):
    levels = np.arange(1, box_edge + 1, dtype=np.float64)
    levels = 2.0 - 2.0 * np.cos(np.pi * levels / (box_edge + 1))
    kept = box_edge * box_edge // LANES
    spare = LANES - box_edge
    low_rows = box_edge - kept
    columns = np.zeros((kept, LANES), np.float64)
    for row in range(kept):
        columns[row, :box_edge] = levels[row] + levels
        part = row // low_rows
        columns[row, box_edge:] = (
            levels[kept + row % low_rows] + levels[part * spare : (part + 1) * spare]
        )
    own = np.repeat(levels[:, None], 2 * LANES, axis=1)
    return columns.astype(np.float32), own.astype(np.float32)


def lane_index(shape):
    return lax.broadcasted_iota(jnp.int32, shape, len(shape) - 1)


def roll_lanes(value, shift):
    return pltpu.roll(value, shift, 1)


def unpack_quad(tiles, edge):
    first, second, third = tiles
    lane = lane_index(first.shape)
    spare = LANES - edge
    keep = lane < edge
    rows = [
        first,
        roll_lanes(jnp.where(lane >= edge, first, second), spare),
        roll_lanes(jnp.where(lane >= edge - spare, second, third), 2 * spare),
        roll_lanes(third, 3 * spare),
    ]
    return [jnp.where(keep, row, 0.0) for row in rows]


def pack_quad(rows, edge):
    zero, one, two, three = rows
    lane = lane_index(zero.shape)
    spare = LANES - edge
    one = roll_lanes(one, edge)
    two = roll_lanes(two, edge - spare)
    three = roll_lanes(three, spare)
    return [
        jnp.where(lane < edge, zero, one),
        jnp.where(lane < edge - spare, one, two),
        jnp.where(lane < spare, two, three),
    ]


def transform_lanes(value, padded_ref):
    high, low = split_bf16(value)
    both = jnp.dot(high, padded_ref[...], preferred_element_type=jnp.float32)
    rest = jnp.dot(low, padded_ref[:, :LANES], preferred_element_type=jnp.float32)
    return both[:, :LANES] + (both[:, LANES:] + rest)


def transform_rows(value, stacked_ref):
    edge = stacked_ref.shape[0] // 2
    high, low = split_bf16(value)
    both = jnp.dot(stacked_ref[...], high, preferred_element_type=jnp.float32)
    rest = jnp.dot(stacked_ref[:edge, :], low, preferred_element_type=jnp.float32)
    return both[:edge] + (both[edge:] + rest)


def prepare_kernel(folds, scalars, dense_ref, boxes_ref, window_ref, buffer):
    orbital_count, edge, _ = dense_ref.shape
    planes = window_ref.shape[2]
    window_planes = REACH * planes
    spread = window_planes - edge
    buffer[...] = jnp.zeros_like(buffer)
    for orbital in range(orbital_count):
        for quad in range(GROUP // 4):
            tiles = [
                dense_ref[orbital, :, (3 * quad + t) * LANES : (3 * quad + t + 1) * LANES]
                for t in range(3)
            ]
            for r, row in enumerate(unpack_quad(tiles, edge)):
                boxes_ref[orbital, 4 * quad + r] = row
    for y in range(GROUP):
        total = None
        for orbital in range(orbital_count):
            row = boxes_ref[orbital, y]
            buffer[orbital, y, spread : spread + edge, :] = roll_lanes(
                row * row, scalars[2 * orbital + 1]
            )
            placed = buffer[orbital, y, pl.ds(spread - scalars[2 * orbital], window_planes), :]
            total = placed if total is None else total + placed
        for _ in range(folds):
            half = total.shape[0] // 2
            total = total[:half] + total[half:]
        for s in range(window_ref.shape[0]):
            window_ref[s, y] = total[s * planes : (s + 1) * planes]


def forward_kernel(
    sub_count, pad, scalars, own_ref, second_ref, dense_ref, padded_ref, stacked_ref, *rest
):
    outs = rest[:sub_count]
    moved_ref, buffer, flat = rest[sub_count:]
    edge = own_ref.shape[2]
    remote = scalars[2]
    buffer[:, :pad, :] = jnp.zeros((GROUP, pad, LANES), jnp.float32)
    buffer[:, pad + edge :, :] = jnp.zeros((GROUP, pad, LANES), jnp.float32)

    @pl.when(remote == 1)
    def _():
        for quad in range(GROUP // 4):
            tiles = [
                dense_ref[:, (3 * quad + t) * LANES : (3 * quad + t + 1) * LANES]
                for t in range(3)
            ]
            for r, row in enumerate(unpack_quad(tiles, edge)):
                buffer[4 * quad + r, pad : pad + edge, :] = row

    @pl.when(remote == 0)
    def _():
        buffer[:, pad : pad + edge, :] = second_ref[0]

    start = pad - scalars[3]
    lane = lane_index((edge, LANES))
    products = []
    for y in range(GROUP):
        moved = roll_lanes(buffer[y, pl.ds(start, edge), :], scalars[4])
        moved = jnp.where(lane < edge, moved, 0.0)
        moved_ref[y] = moved
        products.append(own_ref[0, y] * moved)
    turned = transform_lanes(jnp.concatenate(products, axis=0), padded_ref)
    kept = edge * edge // LANES
    low_rows = edge - kept
    spare = LANES - edge
    keep = lane_index((kept, LANES)) < edge
    for y in range(0, GROUP, 2):
        pair = jnp.concatenate(
            [turned[(y + k) * edge : (y + k + 1) * edge] for k in range(2)], axis=1
        )
        pair = transform_rows(pair, stacked_ref)
        for k in range(2):
            spectral = pair[:, k * LANES : (k + 1) * LANES]
            low = spectral[kept:]
            tail = jnp.concatenate(
                [roll_lanes(low, edge - part * spare) for part in range(kept // low_rows)], axis=0
            )
            flat[pl.ds(y + k, kept, stride=GROUP), :] = jnp.where(keep, spectral[:kept], tail)
    chunk = kept // sub_count * GROUP
    for step in range(sub_count):
        target = partner(scalars[6], step, sub_count)
        outs[step][0] = flat[pl.ds(pl.multiple_of(target * chunk, GROUP), chunk), :]


def solve_kernel(sub_count, groups, scalars, *rest):
    pieces = rest[:sub_count]
    columns_ref, levels_ref, stacked_ref = rest[sub_count : sub_count + 3]
    outs = rest[sub_count + 3 : 2 * sub_count + 3]
    (work,) = rest[2 * sub_count + 3 :]
    count = pieces[0].shape[1] // GROUP
    edge = stacked_ref.shape[0] // 2
    rows = edge // sub_count
    for step in range(sub_count):
        source = partner(scalars[0], step, sub_count)
        for g in range(groups):
            base = pl.multiple_of(source * rows + g * GROUP, GROUP)
            for q in range(count):
                work[q // 2, pl.ds(base, GROUP), (q % 2) * LANES : (q % 2 + 1) * LANES] = pieces[
                    step
                ][g, q * GROUP : (q + 1) * GROUP, :]
    for pair in range(count // 2):
        spectral = transform_rows(work[pair], stacked_ref)
        column = jnp.concatenate(
            [columns_ref[0, 2 * pair + k : 2 * pair + k + 1, :] for k in range(2)], axis=1
        )
        spectral = spectral * ((4.0 * math.pi) / (levels_ref[...] + column + SCREEN))
        work[pair] = transform_rows(spectral, stacked_ref)
    for step in range(sub_count):
        target = partner(scalars[0], step, sub_count)
        for g in range(groups):
            base = pl.multiple_of(target * rows + g * GROUP, GROUP)
            for q in range(count):
                outs[step][g, q * GROUP : (q + 1) * GROUP, :] = work[
                    q // 2, pl.ds(base, GROUP), (q % 2) * LANES : (q % 2 + 1) * LANES
                ]


def backward_kernel(sub_count, pad, scalars, *rest):
    pieces = rest[:sub_count]
    own_ref, moved_ref, padded_ref, stacked_ref, first_ref, second_ref, buffer, flat = rest[
        sub_count:
    ]
    edge = own_ref.shape[2]
    weight = scalars[7].astype(jnp.float32)
    kept = edge * edge // LANES
    low_rows = edge - kept
    spare = LANES - edge
    chunk = kept // sub_count * GROUP
    for step in range(sub_count):
        source = partner(scalars[6], step, sub_count)
        flat[pl.ds(pl.multiple_of(source * chunk, GROUP), chunk), :] = pieces[step][0]
    lane = lane_index((low_rows, LANES))
    turned = []
    for y in range(0, GROUP, 2):
        pair = []
        for k in range(2):
            packed = flat[pl.ds(y + k, kept, stride=GROUP), :]
            low = None
            for part in range(kept // low_rows - 1, -1, -1):
                piece = roll_lanes(
                    packed[part * low_rows : (part + 1) * low_rows], (part + 1) * spare
                )
                low = piece if low is None else jnp.where(lane < (part + 1) * spare, piece, low)
            pair.append(jnp.concatenate([packed, low], axis=0))
        pair = transform_rows(jnp.concatenate(pair, axis=1), stacked_ref)
        turned += [pair[:, :LANES], pair[:, LANES:]]
    potential = transform_lanes(jnp.concatenate(turned, axis=0), padded_ref)
    buffer[:, :pad, :] = jnp.zeros((GROUP, pad, LANES), jnp.float32)
    buffer[:, pad + edge :, :] = jnp.zeros((GROUP, pad, LANES), jnp.float32)
    start = pad + scalars[3]
    for quad in range(GROUP // 4):
        rows = []
        for r in range(4):
            y = 4 * quad + r
            solved = potential[y * edge : (y + 1) * edge] * weight
            first_ref[y] = solved * moved_ref[y]
            buffer[y, pad : pad + edge, :] = solved * own_ref[0, y]
            rows.append(roll_lanes(buffer[y, pl.ds(start, edge), :], scalars[5]))
        for t, tile in enumerate(pack_quad(rows, edge)):
            second_ref[:, (3 * quad + t) * LANES : (3 * quad + t + 1) * LANES] = tile


def combine_kernel(slot_count, fields, folds, scalars, *rest):
    boxes_ref, before_ref, after_ref, low_ref, high_ref = rest[:5]
    field_refs = rest[5 : 5 + fields]
    first_refs = rest[5 + fields : 5 + fields + slot_count]
    second_refs = rest[5 + fields + slot_count : 5 + fields + 2 * slot_count]
    out_ref, buffer, window = rest[5 + fields + 2 * slot_count :]
    orbital_count, _, edge, _ = boxes_ref.shape
    group = pl.program_id(0)
    last = pl.num_programs(0) - 1
    buffer[...] = jnp.zeros_like(buffer)
    position = 0
    planes = field_refs[0].shape[2]
    for ref in field_refs:
        for s in range(ref.shape[0]):
            for copy in range(2**folds):
                start = (position + copy * (REACH // 2**folds)) * planes
                for y in range(GROUP):
                    window[y, start : start + planes, :] = ref[s, y]
            position += 1
    for orbital in range(orbital_count):
        corner = 2 * orbital
        for quad in range(GROUP // 4):
            rows = []
            for r in range(4):
                y = 4 * quad + r
                box = boxes_ref[orbital, y]
                if y == 0:
                    behind = jnp.where(group == 0, low_ref[orbital], before_ref[orbital, 0])
                else:
                    behind = boxes_ref[orbital, y - 1]
                if y == GROUP - 1:
                    ahead = jnp.where(group == last, high_ref[orbital], after_ref[orbital, 0])
                else:
                    ahead = boxes_ref[orbital, y + 1]
                buffer[y % 2, GROUP : GROUP + edge, :] = box
                beside = buffer[y % 2, GROUP - 1 : GROUP - 1 + edge, :]
                beside = beside + buffer[y % 2, GROUP + 1 : GROUP + 1 + edge, :]
                beside = beside + (behind + ahead)
                beside = beside + (roll_lanes(box, 1) + roll_lanes(box, LANES - 1))
                field = window[y, pl.ds(scalars[corner], edge), :]
                field = roll_lanes(field, scalars[corner + 1])
                value = field * box - 0.5 * (beside - 6.0 * box)
                for slot in range(slot_count):
                    share = jnp.where(scalars[2 * orbital_count + slot] == orbital, FOCK_SHARE, 0.0)
                    value = value - share * first_refs[slot][y]
                rows.append(value)
            for t, tile in enumerate(pack_quad(rows, edge)):
                lanes = slice((3 * quad + t) * LANES, (3 * quad + t + 1) * LANES)
                for slot in range(slot_count):
                    local = scalars[2 * orbital_count + slot_count + slot] == orbital
                    tile = tile - jnp.where(local, FOCK_SHARE, 0.0) * second_refs[slot][:, lanes]
                out_ref[orbital, :, lanes] = tile


def whole(shape):
    return pl.BlockSpec(shape, lambda g, s: (0,) * len(shape))


def call(kernel, scalars, operands, in_specs, out_specs, out_shape, scratch, groups, flops):
    return pl.pallas_call(
        kernel,
        grid_spec=pltpu.PrefetchScalarGridSpec(
            num_scalar_prefetch=1,
            grid=(groups,),
            in_specs=in_specs,
            out_specs=out_specs,
            scratch_shapes=scratch,
        ),
        out_shape=out_shape,
        cost_estimate=pl.CostEstimate(flops=flops, bytes_accessed=4_000_000, transcendentals=0),
        compiler_params=pltpu.CompilerParams(dimension_semantics=("arbitrary",)),
    )(scalars, *operands)


def local(orbitals, external_potential, corners, pair_list, pair_count):
    f32 = jnp.float32
    orbital_count, edge, merged = orbitals.shape
    rows = merged // edge
    groups = rows // GROUP
    lanes = GROUP * edge
    devices = lax.axis_size("slab")
    sub_count = lax.axis_size("sub")
    position = lax.axis_index("slab")
    place = lax.axis_index("sub")
    plane_count = external_potential.shape[0]
    grid_planes = plane_count * devices
    spread = REACH * plane_count - edge
    pad = spread + plane_count
    slot_count = pair_list.shape[0]
    total_orbitals = orbital_count * devices
    kept = edge * edge // LANES
    chunk = kept // sub_count * GROUP
    folds = 0
    while (REACH >> (folds + 1)) >= 1 and (REACH >> (folds + 1)) % devices == 0:
        folds += 1
    slabs = REACH >> folds
    padded, stacked = (jnp.asarray(t) for t in sine_tables(edge))
    columns, own_levels = (jnp.asarray(t) for t in level_tables(edge))
    flops = 200_000_000

    asked = from_behind(pair_list, "slab", 1)
    wanted = (asked[:, 1] - position * orbital_count) % total_orbitals
    answers = [
        from_behind(
            lax.dynamic_index_in_dim(
                orbitals, jnp.minimum(wanted[k], orbital_count - 1), 0, keepdims=False
            ),
            "slab",
            -1,
        )
        for k in range(slot_count)
    ]

    own_corners = lax.dynamic_slice_in_dim(corners, position * orbital_count, orbital_count, 0)
    window_start = (own_corners[:, 0] - position * plane_count) % grid_planes
    prepare_scalars = jnp.stack([window_start, own_corners[:, 1]], axis=1).reshape(-1)
    box_shape = (orbital_count, rows, edge, LANES)
    boxes, window = call(
        functools.partial(prepare_kernel, folds),
        prepare_scalars,
        (orbitals,),
        [pl.BlockSpec((orbital_count, edge, lanes), lambda g, s: (0, 0, g))],
        [
            pl.BlockSpec((orbital_count, GROUP, edge, LANES), lambda g, s: (0, g, 0, 0)),
            pl.BlockSpec((slabs, GROUP, plane_count, LANES), lambda g, s: (0, g, 0, 0)),
        ],
        [
            jax.ShapeDtypeStruct(box_shape, f32),
            jax.ShapeDtypeStruct((slabs, rows, plane_count, LANES), f32),
        ],
        [pltpu.VMEM((orbital_count, GROUP, edge + 2 * spread, LANES), f32)],
        groups,
        flops,
    )

    forward = [(i, i + 1) for i in range(sub_count - 1)]
    backward = [(target, source) for source, target in forward]
    low_halo = lax.ppermute(boxes[:, rows - 1], "sub", forward)
    high_halo = lax.ppermute(boxes[:, 0], "sub", backward)

    current = window
    while current.shape[0] > 1:
        half = current.shape[0] // 2
        current = current[:half] + from_behind(current[half:], "slab", half)
    density = current[0].transpose(1, 0, 2).reshape(external_potential.shape)
    local_field = external_potential - LOCAL_FACTOR * jnp.cbrt(density + EPSILON)
    local_field = local_field.reshape(plane_count, rows, LANES).transpose(1, 0, 2)
    fields = [local_field[None]]
    while sum(f.shape[0] for f in fields) < slabs:
        gathered = fields[0] if len(fields) == 1 else jnp.concatenate(fields, axis=0)
        fields.append(from_behind(gathered, "slab", -gathered.shape[0]))

    first_local = (pair_list[:, 0] - position * orbital_count) % total_orbitals
    second_local = (pair_list[:, 1] - position * orbital_count) % total_orbitals
    live = (jnp.arange(slot_count, dtype=jnp.int32) < pair_count[0]).astype(jnp.int32)
    half_span = grid_planes // 2
    corner_first = jnp.take(corners, pair_list[:, 0], axis=0)
    corner_second = jnp.take(corners, pair_list[:, 1], axis=0)
    shift_first = (corner_second[:, 0] - corner_first[:, 0] + half_span) % grid_planes - half_span
    shift_third = corner_second[:, 1] - corner_first[:, 1]
    remote = (second_local >= orbital_count).astype(jnp.int32)
    table = jnp.stack(
        [
            first_local,
            jnp.minimum(second_local, orbital_count - 1),
            remote,
            shift_first,
            shift_third % LANES,
            (-shift_third) % LANES,
            jnp.full((slot_count,), place, jnp.int32),
            live,
        ],
        axis=1,
    ).astype(jnp.int32)

    box_block = (1, GROUP, edge, LANES)
    row_spec = pl.BlockSpec((GROUP, edge, LANES), lambda g, s: (g, 0, 0))
    dense_spec = pl.BlockSpec((edge, lanes), lambda g, s: (0, g))
    piece_spec = pl.BlockSpec((1, chunk, LANES), lambda g, s: (g, 0, 0))
    piece_shape = jax.ShapeDtypeStruct((groups, chunk, LANES), f32)
    own_columns = lax.dynamic_slice_in_dim(columns, place * (kept // sub_count), kept // sub_count)
    shifted = pltpu.VMEM((GROUP, edge + 2 * pad, LANES), f32)
    flat = pltpu.VMEM((kept * GROUP, LANES), f32)
    firsts, seconds, returns = [], [], []
    for slot in range(slot_count):
        scalars = table[slot]
        outs = call(
            functools.partial(forward_kernel, sub_count, pad),
            scalars,
            (boxes, boxes, answers[slot], padded, stacked),
            [
                pl.BlockSpec(box_block, lambda g, s: (s[0], g, 0, 0)),
                pl.BlockSpec(box_block, lambda g, s: (s[1], g, 0, 0)),
                dense_spec,
                whole(padded.shape),
                whole(stacked.shape),
            ],
            [piece_spec] * sub_count + [row_spec],
            [piece_shape] * sub_count + [jax.ShapeDtypeStruct((rows, edge, LANES), f32)],
            [shifted, flat],
            groups,
            flops,
        )
        moved = outs[sub_count]
        pieces = exchange(outs[:sub_count], "sub")
        parts = 3
        tall = chunk // parts
        tall_spec = pl.BlockSpec((groups, tall, LANES), lambda g, s: (0, g, 0))
        solved = call(
            functools.partial(solve_kernel, sub_count, groups),
            place.reshape(1).astype(jnp.int32),
            (*pieces, own_columns.reshape(parts, tall // GROUP, LANES), own_levels, stacked),
            [tall_spec] * sub_count
            + [
                pl.BlockSpec((1, tall // GROUP, LANES), lambda g, s: (g, 0, 0)),
                whole(own_levels.shape),
                whole(stacked.shape),
            ],
            [tall_spec] * sub_count,
            [piece_shape] * sub_count,
            [pltpu.VMEM((tall // GROUP // 2, edge, 2 * LANES), f32)],
            parts,
            flops,
        )
        pieces = exchange(solved, "sub")
        first, second = call(
            functools.partial(backward_kernel, sub_count, pad),
            scalars,
            (*pieces, boxes, moved, padded, stacked),
            [piece_spec] * sub_count
            + [
                pl.BlockSpec(box_block, lambda g, s: (s[0], g, 0, 0)),
                row_spec,
                whole(padded.shape),
                whole(stacked.shape),
            ],
            [row_spec, dense_spec],
            [
                jax.ShapeDtypeStruct((rows, edge, LANES), f32),
                jax.ShapeDtypeStruct((edge, merged), f32),
            ],
            [shifted, flat],
            groups,
            flops,
        )
        firsts.append(first)
        seconds.append(second)
        returns.append(from_behind(second, "slab", 1))

    combine_scalars = jnp.concatenate(
        [
            jnp.stack([window_start, (-own_corners[:, 1]) % LANES], axis=1).reshape(-1),
            first_local,
            second_local,
        ]
    ).astype(jnp.int32)
    edge_block = (orbital_count, 1, edge, LANES)
    partial = call(
        functools.partial(combine_kernel, slot_count, len(fields), folds),
        combine_scalars,
        (boxes, boxes, boxes, low_halo, high_halo, *fields, *firsts, *seconds),
        [
            pl.BlockSpec((orbital_count, GROUP, edge, LANES), lambda g, s: (0, g, 0, 0)),
            pl.BlockSpec(edge_block, lambda g, s: (0, jnp.maximum(g * GROUP - 1, 0), 0, 0)),
            pl.BlockSpec(
                edge_block, lambda g, s: (0, jnp.minimum((g + 1) * GROUP, rows - 1), 0, 0)
            ),
            whole((orbital_count, edge, LANES)),
            whole((orbital_count, edge, LANES)),
        ]
        + [
            pl.BlockSpec((f.shape[0], GROUP, plane_count, LANES), lambda g, s: (0, g, 0, 0))
            for f in fields
        ]
        + [row_spec] * slot_count
        + [dense_spec] * slot_count,
        [pl.BlockSpec((orbital_count, edge, lanes), lambda g, s: (0, 0, g))],
        [jax.ShapeDtypeStruct(orbitals.shape, f32)],
        [
            pltpu.VMEM((2, edge + 2 * GROUP, LANES), f32),
            pltpu.VMEM((GROUP, REACH * plane_count, LANES), f32),
        ],
        groups,
        flops,
    )[0]
    result = partial
    for slot in range(slot_count):
        share = jnp.where(
            wanted[slot] == jnp.arange(orbital_count, dtype=jnp.int32), FOCK_SHARE, 0.0
        )
        result = result - share[:, None, None] * returns[slot][None]
    return result


def solution(mesh):
    placed = (P("slab", None, "sub"), P("slab", "sub"), P(), P("slab", None), P("slab"))
    return jax.shard_map(
        local, mesh=mesh, in_specs=placed, out_specs=P("slab", None, "sub"), check_vma=False
    )
```

```python
import functools
import math

import jax
import jax.numpy as jnp
import numpy as np
from jax import lax
from jax.experimental import pallas as pl
from jax.experimental.pallas import tpu as pltpu
from jax.sharding import PartitionSpec as P

REACH = 16
LANES = 128
GROUP = 8
VMEM_LIMIT = 20 << 20

SCREEN = 0.0008
FOCK_SHARE = 0.25
LOCAL_FACTOR = (3.0 / math.pi) ** (1.0 / 3.0)
EPSILON = 1e-06


def from_behind(value, axis, by):
    size = lax.axis_size(axis)
    return lax.ppermute(value, axis, [(i, (i + by) % size) for i in range(size)])


def partner(index, step, size):
    if size & (size - 1) == 0:
        return index ^ step
    return (size - index + step) % size


def exchange(pieces, axis):
    size = lax.axis_size(axis)
    received = []
    for step, piece in enumerate(pieces):
        pairs = [(i, partner(i, step, size)) for i in range(size)]
        if all(source == target for source, target in pairs):
            received.append(piece)
        else:
            received.append(lax.ppermute(piece, axis, pairs))
    return received


def split_bf16(value):
    high = value.astype(jnp.bfloat16)
    low = (value - high.astype(jnp.float32)).astype(jnp.bfloat16)
    return high, low


def sine_tables(box_edge):
    levels = np.arange(1, box_edge + 1, dtype=np.float64)
    sine = np.sqrt(2.0 / (box_edge + 1)) * np.sin(
        np.pi * levels[:, None] * levels[None, :] / (box_edge + 1)
    )
    sine = sine.astype(np.float32)
    high = sine.astype(jnp.bfloat16)
    low = (sine - high.astype(np.float32)).astype(jnp.bfloat16)
    padded = np.zeros((LANES, 2 * LANES), dtype=high.dtype)
    padded[:box_edge, :box_edge] = high
    padded[:box_edge, LANES : LANES + box_edge] = low
    stacked = np.concatenate([high, low], axis=0)
    return padded, stacked


def level_tables(box_edge):
    levels = np.arange(1, box_edge + 1, dtype=np.float64)
    levels = 2.0 - 2.0 * np.cos(np.pi * levels / (box_edge + 1))
    kept = box_edge * box_edge // LANES
    spare = LANES - box_edge
    low_rows = box_edge - kept
    columns = np.zeros((kept, LANES), np.float64)
    for row in range(kept):
        columns[row, :box_edge] = levels[row] + levels
        part = row // low_rows
        columns[row, box_edge:] = (
            levels[kept + row % low_rows] + levels[part * spare : (part + 1) * spare]
        )
    own = np.repeat(levels[:, None], 2 * LANES, axis=1)
    return columns.astype(np.float32), own.astype(np.float32)


def lane_index(shape):
    return lax.broadcasted_iota(jnp.int32, shape, len(shape) - 1)


def roll_lanes(value, shift):
    return pltpu.roll(value, shift, 1)


def unpack_quad(tiles, edge):
    first, second, third = tiles
    lane = lane_index(first.shape)
    spare = LANES - edge
    keep = lane < edge
    rows = [
        first,
        roll_lanes(jnp.where(lane >= edge, first, second), spare),
        roll_lanes(jnp.where(lane >= edge - spare, second, third), 2 * spare),
        roll_lanes(third, 3 * spare),
    ]
    return [jnp.where(keep, row, 0.0) for row in rows]


def pack_quad(rows, edge):
    zero, one, two, three = rows
    lane = lane_index(zero.shape)
    spare = LANES - edge
    one = roll_lanes(one, edge)
    two = roll_lanes(two, edge - spare)
    three = roll_lanes(three, spare)
    return [
        jnp.where(lane < edge, zero, one),
        jnp.where(lane < edge - spare, one, two),
        jnp.where(lane < spare, two, three),
    ]


def transform_lanes(value, padded_ref):
    high, low = split_bf16(value)
    both = jnp.dot(high, padded_ref[...], preferred_element_type=jnp.float32)
    rest = jnp.dot(low, padded_ref[:, :LANES], preferred_element_type=jnp.float32)
    return both[:, :LANES] + (both[:, LANES:] + rest)


def transform_rows(value, stacked_ref):
    edge = stacked_ref.shape[0] // 2
    high, low = split_bf16(value)
    both = jnp.dot(stacked_ref[...], high, preferred_element_type=jnp.float32)
    rest = jnp.dot(stacked_ref[:edge, :], low, preferred_element_type=jnp.float32)
    return both[:edge] + (both[edge:] + rest)


class Scalars:
    def __init__(self, refs, sizes):
        self.corners, self.pairs, self.count, self.ids = refs
        self.orbital_count, self.plane_count, self.grid_planes = sizes
        self.total = self.corners.shape[0]

    def position(self):
        return self.ids[0]

    def place(self):
        return self.ids[1]

    def window_start(self, orbital):
        first = self.corners[self.position() * self.orbital_count + orbital, 0]
        return lax.rem(
            first - self.position() * self.plane_count + self.grid_planes, self.grid_planes
        )

    def column(self, orbital):
        return self.corners[self.position() * self.orbital_count + orbital, 1]

    def member(self, slot, side):
        owned = self.pairs[slot, side] - self.position() * self.orbital_count
        return lax.rem(owned + self.total, self.total)

    def remote(self, slot):
        return self.member(slot, 1) >= self.orbital_count

    def kept(self, slot):
        return jnp.minimum(self.member(slot, 1), self.orbital_count - 1)

    def shifts(self, slot):
        first, second = self.pairs[slot, 0], self.pairs[slot, 1]
        half = self.grid_planes // 2
        along = self.corners[second, 0] - self.corners[first, 0] + half + self.grid_planes
        return (
            lax.rem(along, self.grid_planes) - half,
            self.corners[second, 1] - self.corners[first, 1],
        )

    def weight(self, slot):
        return jnp.where(slot < self.count[0], 1.0, 0.0).astype(jnp.float32)


def lane_shift(amount):
    return lax.rem(amount + LANES, LANES)


def spread_kernel(sizes, folds, *refs):
    scalars = Scalars(refs[:4], sizes)
    dense_ref, window_ref, buffer = refs[4:]
    orbital_count, edge, _ = dense_ref.shape
    planes = window_ref.shape[2]
    window_planes = REACH * planes
    spread = window_planes - edge

    @pl.when(pl.program_id(0) == 0)
    def _():
        buffer[:, :, :spread, :] = jnp.zeros_like(buffer[:, :, :spread, :])
        buffer[:, :, spread + edge :, :] = jnp.zeros_like(buffer[:, :, spread + edge :, :])

    for orbital in range(orbital_count):
        for quad in range(GROUP // 4):
            tiles = [
                dense_ref[orbital, :, (3 * quad + t) * LANES : (3 * quad + t + 1) * LANES]
                for t in range(3)
            ]
            for r, row in enumerate(unpack_quad(tiles, edge)):
                buffer[orbital, 4 * quad + r, spread : spread + edge, :] = roll_lanes(
                    row * row, scalars.column(orbital)
                )
    for y in range(GROUP):
        total = None
        for orbital in range(orbital_count):
            start = spread - scalars.window_start(orbital)
            placed = buffer[orbital, y, pl.ds(start, window_planes), :]
            total = placed if total is None else total + placed
        for _ in range(folds):
            half = total.shape[0] // 2
            total = total[:half] + total[half:]
        for s in range(window_ref.shape[0]):
            window_ref[s, y] = total[s * planes : (s + 1) * planes]


def unpack_kernel(dense_ref, boxes_ref):
    orbital_count, edge, _ = dense_ref.shape
    for orbital in range(orbital_count):
        for quad in range(GROUP // 4):
            tiles = [
                dense_ref[orbital, :, (3 * quad + t) * LANES : (3 * quad + t + 1) * LANES]
                for t in range(3)
            ]
            for r, row in enumerate(unpack_quad(tiles, edge)):
                boxes_ref[orbital, 4 * quad + r] = row


def forward_kernel(sizes, sub_count, pad, slot, *refs):
    scalars = Scalars(refs[:4], sizes)
    own_ref, second_ref, dense_ref, padded_ref, stacked_ref = refs[4:9]
    outs = refs[9 : 9 + sub_count]
    moved_ref, buffer, flat = refs[9 + sub_count :]
    edge = own_ref.shape[2]
    remote = scalars.remote(slot)

    @pl.when(pl.program_id(0) == 0)
    def _():
        buffer[:, :pad, :] = jnp.zeros((GROUP, pad, LANES), jnp.float32)
        buffer[:, pad + edge :, :] = jnp.zeros((GROUP, pad, LANES), jnp.float32)

    @pl.when(remote)
    def _():
        for quad in range(GROUP // 4):
            tiles = [
                dense_ref[:, (3 * quad + t) * LANES : (3 * quad + t + 1) * LANES]
                for t in range(3)
            ]
            for r, row in enumerate(unpack_quad(tiles, edge)):
                buffer[4 * quad + r, pad : pad + edge, :] = row

    @pl.when(jnp.logical_not(remote))
    def _():
        buffer[:, pad : pad + edge, :] = second_ref[0]

    along, across = scalars.shifts(slot)
    lane = lane_index((edge, LANES))
    products = []
    for y in range(GROUP):
        moved = roll_lanes(buffer[y, pl.ds(pad - along, edge), :], lane_shift(across))
        moved = jnp.where(lane < edge, moved, 0.0)
        moved_ref[y] = moved
        products.append(own_ref[0, y] * moved)
    turned = transform_lanes(jnp.concatenate(products, axis=0), padded_ref)
    kept = edge * edge // LANES
    low_rows = edge - kept
    spare = LANES - edge
    keep = lane_index((kept, LANES)) < edge
    for y in range(0, GROUP, 2):
        pair = jnp.concatenate(
            [turned[(y + k) * edge : (y + k + 1) * edge] for k in range(2)], axis=1
        )
        pair = transform_rows(pair, stacked_ref)
        for k in range(2):
            spectral = pair[:, k * LANES : (k + 1) * LANES]
            low = spectral[kept:]
            tail = jnp.concatenate(
                [roll_lanes(low, edge - part * spare) for part in range(kept // low_rows)], axis=0
            )
            flat[pl.ds(y + k, kept, stride=GROUP), :] = jnp.where(keep, spectral[:kept], tail)
    chunk = kept // sub_count * GROUP
    for step in range(sub_count):
        target = partner(scalars.place(), step, sub_count)
        outs[step][0] = flat[pl.ds(pl.multiple_of(target * chunk, GROUP), chunk), :]


def solve_kernel(sizes, sub_count, groups, *refs):
    scalars = Scalars(refs[:4], sizes)
    rest = refs[4:]
    pieces = rest[:sub_count]
    columns_ref, levels_ref, stacked_ref = rest[sub_count : sub_count + 3]
    outs = rest[sub_count + 3 : 2 * sub_count + 3]
    (work,) = rest[2 * sub_count + 3 :]
    count = pieces[0].shape[1] // GROUP
    edge = stacked_ref.shape[0] // 2
    rows = edge // sub_count
    for step in range(sub_count):
        source = partner(scalars.place(), step, sub_count)
        for g in range(groups):
            base = pl.multiple_of(source * rows + g * GROUP, GROUP)
            for q in range(count):
                work[q // 2, pl.ds(base, GROUP), (q % 2) * LANES : (q % 2 + 1) * LANES] = pieces[
                    step
                ][g, q * GROUP : (q + 1) * GROUP, :]
    first = scalars.place() * (count * pl.num_programs(0)) + pl.program_id(0) * count
    for pair in range(count // 2):
        spectral = transform_rows(work[pair], stacked_ref)
        column = jnp.concatenate(
            [columns_ref[pl.ds(first + 2 * pair + k, 1), :] for k in range(2)], axis=1
        )
        spectral = spectral * ((4.0 * math.pi) / (levels_ref[...] + column + SCREEN))
        work[pair] = transform_rows(spectral, stacked_ref)
    for step in range(sub_count):
        target = partner(scalars.place(), step, sub_count)
        for g in range(groups):
            base = pl.multiple_of(target * rows + g * GROUP, GROUP)
            for q in range(count):
                outs[step][g, q * GROUP : (q + 1) * GROUP, :] = work[
                    q // 2, pl.ds(base, GROUP), (q % 2) * LANES : (q % 2 + 1) * LANES
                ]


def backward_kernel(sizes, sub_count, pad, slot, *refs):
    scalars = Scalars(refs[:4], sizes)
    rest = refs[4:]
    pieces = rest[:sub_count]
    own_ref, moved_ref, padded_ref, stacked_ref, first_ref, second_ref, buffer, flat = rest[
        sub_count:
    ]
    edge = own_ref.shape[2]
    weight = scalars.weight(slot)
    kept = edge * edge // LANES
    low_rows = edge - kept
    spare = LANES - edge
    chunk = kept // sub_count * GROUP

    @pl.when(pl.program_id(0) == 0)
    def _():
        buffer[:, :pad, :] = jnp.zeros((GROUP, pad, LANES), jnp.float32)
        buffer[:, pad + edge :, :] = jnp.zeros((GROUP, pad, LANES), jnp.float32)

    for step in range(sub_count):
        source = partner(scalars.place(), step, sub_count)
        flat[pl.ds(pl.multiple_of(source * chunk, GROUP), chunk), :] = pieces[step][0]
    lane = lane_index((low_rows, LANES))
    turned = []
    for y in range(0, GROUP, 2):
        pair = []
        for k in range(2):
            packed = flat[pl.ds(y + k, kept, stride=GROUP), :]
            low = None
            for part in range(kept // low_rows - 1, -1, -1):
                piece = roll_lanes(
                    packed[part * low_rows : (part + 1) * low_rows], (part + 1) * spare
                )
                low = piece if low is None else jnp.where(lane < (part + 1) * spare, piece, low)
            pair.append(jnp.concatenate([packed, low], axis=0))
        pair = transform_rows(jnp.concatenate(pair, axis=1), stacked_ref)
        turned += [pair[:, :LANES], pair[:, LANES:]]
    potential = transform_lanes(jnp.concatenate(turned, axis=0), padded_ref)
    along, across = scalars.shifts(slot)
    for quad in range(GROUP // 4):
        rows = []
        for r in range(4):
            y = 4 * quad + r
            solved = potential[y * edge : (y + 1) * edge] * weight
            first_ref[y] = solved * moved_ref[y]
            buffer[y, pad : pad + edge, :] = solved * own_ref[0, y]
            rows.append(roll_lanes(buffer[y, pl.ds(pad + along, edge), :], lane_shift(-across)))
        for t, tile in enumerate(pack_quad(rows, edge)):
            second_ref[:, (3 * quad + t) * LANES : (3 * quad + t + 1) * LANES] = tile


def combine_kernel(sizes, slot_count, fields, folds, *refs):
    scalars = Scalars(refs[:4], sizes)
    rest = refs[4:]
    boxes_ref, before_ref, after_ref, low_ref, high_ref = rest[:5]
    field_refs = rest[5 : 5 + fields]
    first_refs = rest[5 + fields : 5 + fields + slot_count]
    second_refs = rest[5 + fields + slot_count : 5 + fields + 2 * slot_count]
    out_ref, buffer, window = rest[5 + fields + 2 * slot_count :]
    orbital_count, _, edge, _ = boxes_ref.shape
    group = pl.program_id(0)
    last = pl.num_programs(0) - 1
    buffer[...] = jnp.zeros_like(buffer)
    position = 0
    planes = field_refs[0].shape[2]
    half = (fields - 1) // 2
    sources = [field_refs[:1]] + [(field_refs[1 + k], field_refs[1 + half + k]) for k in range(half)]
    for refs_ in sources:
        for s in range(refs_[0].shape[0]):
            for y in range(GROUP):
                value = refs_[0][s, y]
                for ref in refs_[1:]:
                    value = value + ref[s, y]
                for copy in range(2**folds):
                    start = (position + copy * (REACH // 2**folds)) * planes
                    window[y, start : start + planes, :] = value
            position += 1
    for orbital in range(orbital_count):
        begin = scalars.window_start(orbital)
        turn = lane_shift(-scalars.column(orbital))
        shares = [
            jnp.where(scalars.member(slot, 0) == orbital, FOCK_SHARE, 0.0)
            for slot in range(slot_count)
        ]
        locals_ = [
            jnp.where(scalars.member(slot, 1) == orbital, FOCK_SHARE, 0.0)
            for slot in range(slot_count)
        ]
        for quad in range(GROUP // 4):
            rows = []
            for r in range(4):
                y = 4 * quad + r
                box = boxes_ref[orbital, y]
                if y == 0:
                    behind = jnp.where(group == 0, low_ref[orbital], before_ref[orbital, 0])
                else:
                    behind = boxes_ref[orbital, y - 1]
                if y == GROUP - 1:
                    ahead = jnp.where(group == last, high_ref[orbital], after_ref[orbital, 0])
                else:
                    ahead = boxes_ref[orbital, y + 1]
                buffer[y % 2, GROUP : GROUP + edge, :] = box
                beside = buffer[y % 2, GROUP - 1 : GROUP - 1 + edge, :]
                beside = beside + buffer[y % 2, GROUP + 1 : GROUP + 1 + edge, :]
                beside = beside + (behind + ahead)
                beside = beside + (roll_lanes(box, 1) + roll_lanes(box, LANES - 1))
                field = roll_lanes(window[y, pl.ds(begin, edge), :], turn)
                value = field * box - 0.5 * (beside - 6.0 * box)
                for slot in range(slot_count):
                    value = value - shares[slot] * first_refs[slot][y]
                rows.append(value)
            for t, tile in enumerate(pack_quad(rows, edge)):
                lanes = slice((3 * quad + t) * LANES, (3 * quad + t + 1) * LANES)
                for slot in range(slot_count):
                    tile = tile - locals_[slot] * second_refs[slot][:, lanes]
                out_ref[orbital, :, lanes] = tile


def whole(shape):
    return pl.BlockSpec(shape, lambda g, *s: (0,) * len(shape))


def call(kernel, scalars, operands, in_specs, out_specs, out_shape, scratch, groups, flops):
    return pl.pallas_call(
        kernel,
        grid_spec=pltpu.PrefetchScalarGridSpec(
            num_scalar_prefetch=len(scalars),
            grid=(groups,),
            in_specs=in_specs,
            out_specs=out_specs,
            scratch_shapes=scratch,
        ),
        out_shape=out_shape,
        cost_estimate=pl.CostEstimate(
            flops=flops, bytes_accessed=4_000_000, transcendentals=0
        ),
        compiler_params=pltpu.CompilerParams(
            dimension_semantics=("arbitrary",), vmem_limit_bytes=VMEM_LIMIT
        ),
    )(*scalars, *operands)


def program(orbitals, external_potential, corners, pair_list, pair_count):
    f32 = jnp.float32
    orbital_count, edge, merged = orbitals.shape
    rows = merged // edge
    groups = rows // GROUP
    lanes = GROUP * edge
    devices = lax.axis_size("slab")
    sub_count = lax.axis_size("sub")
    position = lax.axis_index("slab")
    place = lax.axis_index("sub")
    plane_count = external_potential.shape[0]
    grid_planes = plane_count * devices
    sizes = (orbital_count, plane_count, grid_planes)
    spread = REACH * plane_count - edge
    pad = spread + plane_count
    slot_count = pair_list.shape[0]
    kept = edge * edge // LANES
    chunk = kept // sub_count * GROUP
    folds = 0
    while (REACH >> (folds + 1)) >= 2 and (REACH >> (folds + 1)) % devices == 0:
        folds += 1
    slabs = REACH >> folds
    padded, stacked = (jnp.asarray(t) for t in sine_tables(edge))
    columns, own_levels = (jnp.asarray(t) for t in level_tables(edge))
    flops = 200_000_000
    ids = jnp.stack([position, place]).astype(jnp.int32)
    scalars = (corners, pair_list, pair_count, ids)

    asked = from_behind(pair_list, "slab", 1)

    box_shape = (orbital_count, rows, edge, LANES)
    own_spec = pl.BlockSpec((orbital_count, edge, lanes), lambda g, *s: (0, 0, g))
    window = call(
        functools.partial(spread_kernel, sizes, folds),
        scalars,
        (orbitals,),
        [own_spec],
        [pl.BlockSpec((slabs, GROUP, plane_count, LANES), lambda g, *s: (0, g, 0, 0))],
        [jax.ShapeDtypeStruct((slabs, rows, plane_count, LANES), f32)],
        [pltpu.VMEM((orbital_count, GROUP, edge + 2 * spread, LANES), f32)],
        groups,
        flops,
    )[0]
    boxes = call(
        unpack_kernel,
        (),
        (orbitals,),
        [own_spec],
        [pl.BlockSpec((orbital_count, GROUP, edge, LANES), lambda g, *s: (0, g, 0, 0))],
        [jax.ShapeDtypeStruct(box_shape, f32)],
        [],
        groups,
        flops,
    )[0]

    near = window[:2]
    parts = []
    for hop in range(2, slabs, 2):
        parts.append(from_behind(window[hop : hop + 2], "slab", hop))
    for part in parts:
        near = near + part
    onward = from_behind(near[1], "slab", 1)
    density = (near[0] + onward).transpose(1, 0, 2).reshape(external_potential.shape)
    local_field = external_potential - LOCAL_FACTOR * jnp.cbrt(density + EPSILON)
    local_field = local_field.reshape(plane_count, rows, LANES).transpose(1, 0, 2)
    beyond = from_behind(local_field, "slab", -1)
    both = jnp.stack([local_field, beyond])
    fields = [both]
    for parity in (1, 0):
        for hop in range(2, slabs, 2):
            pairs = [(i, (i - hop) % devices) for i in range(parity, devices, 2)]
            fields.append(lax.ppermute(both, "slab", pairs))

    answers = []
    for k in range(slot_count):
        picked = lax.dynamic_index_in_dim(
            orbitals, lax.rem(asked[k, 1], orbital_count), 0, keepdims=False
        )
        answers.append(from_behind(picked, "slab", -1))

    forward = [(i, i + 1) for i in range(sub_count - 1)]
    backward = [(target, source) for source, target in forward]
    low_halo = lax.ppermute(boxes[:, rows - 1], "sub", forward)
    high_halo = lax.ppermute(boxes[:, 0], "sub", backward)

    def side(slot, pick):
        def index(g, c, p, n, d):
            scalar = Scalars((c, p, n, d), sizes)
            return (scalar.kept(slot) if pick else scalar.member(slot, 0), g, 0, 0)

        return pl.BlockSpec((1, GROUP, edge, LANES), index)

    row_spec = pl.BlockSpec((GROUP, edge, LANES), lambda g, *s: (g, 0, 0))
    dense_spec = pl.BlockSpec((edge, lanes), lambda g, *s: (0, g))
    piece_spec = pl.BlockSpec((1, chunk, LANES), lambda g, *s: (g, 0, 0))
    piece_shape = jax.ShapeDtypeStruct((groups, chunk, LANES), f32)
    shifted = pltpu.VMEM((GROUP, edge + 2 * pad, LANES), f32)
    flat = pltpu.VMEM((kept * GROUP, LANES), f32)
    solve_steps = 3
    tall = chunk // solve_steps
    tall_spec = pl.BlockSpec((groups, tall, LANES), lambda g, *s: (0, g, 0))
    firsts, seconds, returns = [], [], []
    for slot in range(slot_count):
        outs = call(
            functools.partial(forward_kernel, sizes, sub_count, pad, slot),
            scalars,
            (boxes, boxes, answers[slot], padded, stacked),
            [side(slot, 0), side(slot, 1), dense_spec, whole(padded.shape), whole(stacked.shape)],
            [piece_spec] * sub_count + [row_spec],
            [piece_shape] * sub_count + [jax.ShapeDtypeStruct((rows, edge, LANES), f32)],
            [shifted, flat],
            groups,
            flops,
        )
        moved = outs[sub_count]
        pieces = exchange(outs[:sub_count], "sub")
        solved = call(
            functools.partial(solve_kernel, sizes, sub_count, groups),
            scalars,
            (*pieces, columns, own_levels, stacked),
            [tall_spec] * sub_count
            + [whole(columns.shape), whole(own_levels.shape), whole(stacked.shape)],
            [tall_spec] * sub_count,
            [piece_shape] * sub_count,
            [pltpu.VMEM((tall // GROUP // 2, edge, 2 * LANES), f32)],
            solve_steps,
            flops,
        )
        pieces = exchange(solved, "sub")
        first, second = call(
            functools.partial(backward_kernel, sizes, sub_count, pad, slot),
            scalars,
            (*pieces, boxes, moved, padded, stacked),
            [piece_spec] * sub_count
            + [side(slot, 0), row_spec, whole(padded.shape), whole(stacked.shape)],
            [row_spec, dense_spec],
            [
                jax.ShapeDtypeStruct((rows, edge, LANES), f32),
                jax.ShapeDtypeStruct((edge, merged), f32),
            ],
            [shifted, flat],
            groups,
            flops,
        )
        firsts.append(first)
        seconds.append(second)
        returns.append(from_behind(second, "slab", 1))

    edge_block = (orbital_count, 1, edge, LANES)
    partial = call(
        functools.partial(combine_kernel, sizes, slot_count, len(fields), folds),
        scalars,
        (boxes, boxes, boxes, low_halo, high_halo, *fields, *firsts, *seconds),
        [
            pl.BlockSpec((orbital_count, GROUP, edge, LANES), lambda g, *s: (0, g, 0, 0)),
            pl.BlockSpec(edge_block, lambda g, *s: (0, jnp.maximum(g * GROUP - 1, 0), 0, 0)),
            pl.BlockSpec(
                edge_block, lambda g, *s: (0, jnp.minimum((g + 1) * GROUP, rows - 1), 0, 0)
            ),
            whole((orbital_count, edge, LANES)),
            whole((orbital_count, edge, LANES)),
        ]
        + [
            pl.BlockSpec((f.shape[0], GROUP, plane_count, LANES), lambda g, *s: (0, g, 0, 0))
            for f in fields
        ]
        + [row_spec] * slot_count
        + [dense_spec] * slot_count,
        [pl.BlockSpec((orbital_count, edge, lanes), lambda g, *s: (0, 0, g))],
        [jax.ShapeDtypeStruct(orbitals.shape, f32)],
        [
            pltpu.VMEM((2, edge + 2 * GROUP, LANES), f32),
            pltpu.VMEM((GROUP, REACH * plane_count, LANES), f32),
        ],
        groups,
        flops,
    )[0]
    result = partial
    for slot in range(slot_count):
        share = jnp.where(
            asked[slot, 1] == position * orbital_count + jnp.arange(orbital_count),
            FOCK_SHARE,
            0.0,
        )
        result = result - share[:, None, None] * returns[slot][None]
    return result


def solution(mesh):
    placed = (P("slab", None, "sub"), P("slab", "sub"), P(), P("slab", None), P("slab"))
    return jax.shard_map(
        program, mesh=mesh, in_specs=placed, out_specs=P("slab", None, "sub"), check_vma=False
    )
```

```python
import functools
import math

import jax
import jax.numpy as jnp
import numpy as np
from jax import lax
from jax.experimental import pallas as pl
from jax.experimental.pallas import tpu as pltpu
from jax.sharding import PartitionSpec as P

REACH = 16
LANES = 128
GROUP = 8
VMEM_LIMIT = 20 << 20

SCREEN = 0.0008
FOCK_SHARE = 0.25
LOCAL_FACTOR = (3.0 / math.pi) ** (1.0 / 3.0)
EPSILON = 1e-06


def from_behind(value, axis, by):
    size = lax.axis_size(axis)
    return lax.ppermute(value, axis, [(i, (i + by) % size) for i in range(size)])


def partner(index, step, size):
    if size & (size - 1) == 0:
        return index ^ step
    return (size - index + step) % size


def exchange(pieces, axis):
    size = lax.axis_size(axis)
    received = []
    for step, piece in enumerate(pieces):
        pairs = [(i, partner(i, step, size)) for i in range(size)]
        if all(source == target for source, target in pairs):
            received.append(piece)
        else:
            received.append(lax.ppermute(piece, axis, pairs))
    return received


def split_bf16(value):
    high = value.astype(jnp.bfloat16)
    low = (value - high.astype(jnp.float32)).astype(jnp.bfloat16)
    return high, low


def sine_tables(box_edge):
    levels = np.arange(1, box_edge + 1, dtype=np.float64)
    sine = np.sqrt(2.0 / (box_edge + 1)) * np.sin(
        np.pi * levels[:, None] * levels[None, :] / (box_edge + 1)
    )
    sine = sine.astype(np.float32)
    high = sine.astype(jnp.bfloat16)
    low = (sine - high.astype(np.float32)).astype(jnp.bfloat16)
    padded = np.zeros((LANES, 2 * LANES), dtype=high.dtype)
    padded[:box_edge, :box_edge] = high
    padded[:box_edge, LANES : LANES + box_edge] = low
    stacked = np.concatenate([high, low], axis=0)
    return padded, stacked


def level_tables(box_edge):
    levels = np.arange(1, box_edge + 1, dtype=np.float64)
    levels = 2.0 - 2.0 * np.cos(np.pi * levels / (box_edge + 1))
    kept = box_edge * box_edge // LANES
    spare = LANES - box_edge
    low_rows = box_edge - kept
    columns = np.zeros((kept, LANES), np.float64)
    for row in range(kept):
        columns[row, :box_edge] = levels[row] + levels
        part = row // low_rows
        columns[row, box_edge:] = (
            levels[kept + row % low_rows] + levels[part * spare : (part + 1) * spare]
        )
    own = np.repeat(levels[:, None], 2 * LANES, axis=1)
    return columns.astype(np.float32), own.astype(np.float32)


def lane_index(shape):
    return lax.broadcasted_iota(jnp.int32, shape, len(shape) - 1)


def roll_lanes(value, shift):
    return pltpu.roll(value, shift, 1)


def unpack_quad(tiles, edge):
    first, second, third = tiles
    lane = lane_index(first.shape)
    spare = LANES - edge
    keep = lane < edge
    rows = [
        first,
        roll_lanes(jnp.where(lane >= edge, first, second), spare),
        roll_lanes(jnp.where(lane >= edge - spare, second, third), 2 * spare),
        roll_lanes(third, 3 * spare),
    ]
    return [jnp.where(keep, row, 0.0) for row in rows]


def pack_quad(rows, edge):
    zero, one, two, three = rows
    lane = lane_index(zero.shape)
    spare = LANES - edge
    one = roll_lanes(one, edge)
    two = roll_lanes(two, edge - spare)
    three = roll_lanes(three, spare)
    return [
        jnp.where(lane < edge, zero, one),
        jnp.where(lane < edge - spare, one, two),
        jnp.where(lane < spare, two, three),
    ]


def transform_lanes(value, padded_ref):
    high, low = split_bf16(value)
    both = jnp.dot(high, padded_ref[...], preferred_element_type=jnp.float32)
    rest = jnp.dot(low, padded_ref[:, :LANES], preferred_element_type=jnp.float32)
    return both[:, :LANES] + (both[:, LANES:] + rest)


def transform_rows(value, stacked_ref):
    edge = stacked_ref.shape[0] // 2
    high, low = split_bf16(value)
    both = jnp.dot(stacked_ref[...], high, preferred_element_type=jnp.float32)
    rest = jnp.dot(stacked_ref[:edge, :], low, preferred_element_type=jnp.float32)
    return both[:edge] + (both[edge:] + rest)


class Scalars:
    def __init__(self, refs, sizes):
        self.corners, self.pairs, self.count, self.ids = refs
        self.orbital_count, self.plane_count, self.grid_planes = sizes
        self.total = self.corners.shape[0]

    def position(self):
        return self.ids[0]

    def place(self):
        return self.ids[1]

    def window_start(self, orbital):
        first = self.corners[self.position() * self.orbital_count + orbital, 0]
        return lax.rem(
            first - self.position() * self.plane_count + self.grid_planes, self.grid_planes
        )

    def column(self, orbital):
        return self.corners[self.position() * self.orbital_count + orbital, 1]

    def member(self, slot, side):
        owned = self.pairs[slot, side] - self.position() * self.orbital_count
        return lax.rem(owned + self.total, self.total)

    def remote(self, slot):
        return self.member(slot, 1) >= self.orbital_count

    def kept(self, slot):
        return jnp.minimum(self.member(slot, 1), self.orbital_count - 1)

    def shifts(self, slot):
        first, second = self.pairs[slot, 0], self.pairs[slot, 1]
        half = self.grid_planes // 2
        along = self.corners[second, 0] - self.corners[first, 0] + half + self.grid_planes
        return (
            lax.rem(along, self.grid_planes) - half,
            self.corners[second, 1] - self.corners[first, 1],
        )

    def weight(self, slot):
        return jnp.where(slot < self.count[0], 1.0, 0.0).astype(jnp.float32)


def lane_shift(amount):
    return lax.rem(amount + LANES, LANES)


def spread_kernel(sizes, folds, corners, ids, dense_ref, *refs):
    scalars = Scalars((corners, None, None, ids), sizes)
    *window_refs, buffer = refs
    orbital_count, edge, _ = dense_ref.shape
    planes = window_refs[0].shape[2]
    window_planes = REACH * planes
    spread = window_planes - edge

    @pl.when(pl.program_id(0) == 0)
    def _():
        buffer[:, :, :spread, :] = jnp.zeros_like(buffer[:, :, :spread, :])
        buffer[:, :, spread + edge :, :] = jnp.zeros_like(buffer[:, :, spread + edge :, :])

    for orbital in range(orbital_count):
        for quad in range(GROUP // 4):
            tiles = [
                dense_ref[orbital, :, (3 * quad + t) * LANES : (3 * quad + t + 1) * LANES]
                for t in range(3)
            ]
            for r, row in enumerate(unpack_quad(tiles, edge)):
                buffer[orbital, 4 * quad + r, spread : spread + edge, :] = roll_lanes(
                    row * row, scalars.column(orbital)
                )
    for y in range(GROUP):
        total = None
        for orbital in range(orbital_count):
            start = spread - scalars.window_start(orbital)
            placed = buffer[orbital, y, pl.ds(start, window_planes), :]
            total = placed if total is None else total + placed
        for _ in range(folds):
            half = total.shape[0] // 2
            total = total[:half] + total[half:]
        for s in range(2 * len(window_refs)):
            window_refs[s // 2][s % 2, y] = total[s * planes : (s + 1) * planes]


def unpack_kernel(dense_ref, boxes_ref):
    orbital_count, edge, _ = dense_ref.shape
    for orbital in range(orbital_count):
        for quad in range(GROUP // 4):
            tiles = [
                dense_ref[orbital, :, (3 * quad + t) * LANES : (3 * quad + t + 1) * LANES]
                for t in range(3)
            ]
            for r, row in enumerate(unpack_quad(tiles, edge)):
                boxes_ref[orbital, 4 * quad + r] = row


def forward_kernel(sizes, sub_count, pad, slot, *refs):
    scalars = Scalars(refs[:4], sizes)
    own_ref, second_ref, dense_ref, padded_ref, stacked_ref = refs[4:9]
    outs = refs[9 : 9 + sub_count]
    moved_ref, buffer, flat = refs[9 + sub_count :]
    edge = own_ref.shape[2]
    remote = scalars.remote(slot)

    @pl.when(pl.program_id(0) == 0)
    def _():
        buffer[:, :pad, :] = jnp.zeros((GROUP, pad, LANES), jnp.float32)
        buffer[:, pad + edge :, :] = jnp.zeros((GROUP, pad, LANES), jnp.float32)

    @pl.when(remote)
    def _():
        for quad in range(GROUP // 4):
            tiles = [
                dense_ref[:, (3 * quad + t) * LANES : (3 * quad + t + 1) * LANES]
                for t in range(3)
            ]
            for r, row in enumerate(unpack_quad(tiles, edge)):
                buffer[4 * quad + r, pad : pad + edge, :] = row

    @pl.when(jnp.logical_not(remote))
    def _():
        buffer[:, pad : pad + edge, :] = second_ref[0]

    along, across = scalars.shifts(slot)
    lane = lane_index((edge, LANES))
    products = []
    for y in range(GROUP):
        moved = roll_lanes(buffer[y, pl.ds(pad - along, edge), :], lane_shift(across))
        moved = jnp.where(lane < edge, moved, 0.0)
        moved_ref[y] = moved
        products.append(own_ref[0, y] * moved)
    turned = transform_lanes(jnp.concatenate(products, axis=0), padded_ref)
    kept = edge * edge // LANES
    low_rows = edge - kept
    spare = LANES - edge
    keep = lane_index((kept, LANES)) < edge
    for y in range(0, GROUP, 2):
        pair = jnp.concatenate(
            [turned[(y + k) * edge : (y + k + 1) * edge] for k in range(2)], axis=1
        )
        pair = transform_rows(pair, stacked_ref)
        for k in range(2):
            spectral = pair[:, k * LANES : (k + 1) * LANES]
            low = spectral[kept:]
            tail = jnp.concatenate(
                [roll_lanes(low, edge - part * spare) for part in range(kept // low_rows)], axis=0
            )
            flat[pl.ds(y + k, kept, stride=GROUP), :] = jnp.where(keep, spectral[:kept], tail)
    chunk = kept // sub_count * GROUP
    for step in range(sub_count):
        target = partner(scalars.place(), step, sub_count)
        outs[step][0] = flat[pl.ds(pl.multiple_of(target * chunk, GROUP), chunk), :]


def solve_kernel(sizes, sub_count, groups, parts, *refs):
    scalars = Scalars(refs[:4], sizes)
    rest = refs[4:]
    pieces = rest[:sub_count]
    columns_ref, levels_ref, stacked_ref = rest[sub_count : sub_count + 3]
    outs = rest[sub_count + 3 : -1]
    work = rest[-1]
    count = pieces[0].shape[1] // GROUP
    edge = stacked_ref.shape[0] // 2
    rows = edge // sub_count
    for step in range(sub_count):
        source = partner(scalars.place(), step, sub_count)
        for g in range(groups):
            base = pl.multiple_of(source * rows + g * GROUP, GROUP)
            for q in range(count):
                work[q // 2, pl.ds(base, GROUP), (q % 2) * LANES : (q % 2 + 1) * LANES] = pieces[
                    step
                ][g, q * GROUP : (q + 1) * GROUP, :]
    first = scalars.place() * (count * pl.num_programs(0)) + pl.program_id(0) * count
    for pair in range(count // 2):
        spectral = transform_rows(work[pair], stacked_ref)
        column = jnp.concatenate(
            [columns_ref[pl.ds(first + 2 * pair + k, 1), :] for k in range(2)], axis=1
        )
        spectral = spectral * ((4.0 * math.pi) / (levels_ref[...] + column + SCREEN))
        work[pair] = transform_rows(spectral, stacked_ref)
    for step in range(sub_count):
        target = partner(scalars.place(), step, sub_count)
        for part, (first_group, group_count) in enumerate(parts):
            out = outs[part * sub_count + step]
            for g in range(group_count):
                base = pl.multiple_of(target * rows + (first_group + g) * GROUP, GROUP)
                for q in range(count):
                    out[g, q * GROUP : (q + 1) * GROUP, :] = work[
                        q // 2, pl.ds(base, GROUP), (q % 2) * LANES : (q % 2 + 1) * LANES
                    ]


def backward_kernel(sizes, sub_count, pad, slot, *refs):
    scalars = Scalars(refs[:4], sizes)
    rest = refs[4:]
    pieces = rest[:sub_count]
    own_ref, moved_ref, padded_ref, stacked_ref, first_ref, second_ref, buffer, flat = rest[
        sub_count:
    ]
    edge = own_ref.shape[2]
    weight = scalars.weight(slot)
    kept = edge * edge // LANES
    low_rows = edge - kept
    spare = LANES - edge
    chunk = kept // sub_count * GROUP

    @pl.when(pl.program_id(0) == 0)
    def _():
        buffer[:, :pad, :] = jnp.zeros((GROUP, pad, LANES), jnp.float32)
        buffer[:, pad + edge :, :] = jnp.zeros((GROUP, pad, LANES), jnp.float32)

    for step in range(sub_count):
        source = partner(scalars.place(), step, sub_count)
        flat[pl.ds(pl.multiple_of(source * chunk, GROUP), chunk), :] = pieces[step][0]
    lane = lane_index((low_rows, LANES))
    turned = []
    for y in range(0, GROUP, 2):
        pair = []
        for k in range(2):
            packed = flat[pl.ds(y + k, kept, stride=GROUP), :]
            low = None
            for part in range(kept // low_rows - 1, -1, -1):
                piece = roll_lanes(
                    packed[part * low_rows : (part + 1) * low_rows], (part + 1) * spare
                )
                low = piece if low is None else jnp.where(lane < (part + 1) * spare, piece, low)
            pair.append(jnp.concatenate([packed, low], axis=0))
        pair = transform_rows(jnp.concatenate(pair, axis=1), stacked_ref)
        turned += [pair[:, :LANES], pair[:, LANES:]]
    potential = transform_lanes(jnp.concatenate(turned, axis=0), padded_ref)
    along, across = scalars.shifts(slot)
    for quad in range(GROUP // 4):
        rows = []
        for r in range(4):
            y = 4 * quad + r
            solved = potential[y * edge : (y + 1) * edge] * weight
            first_ref[y] = solved * moved_ref[y]
            buffer[y, pad : pad + edge, :] = solved * own_ref[0, y]
            rows.append(roll_lanes(buffer[y, pl.ds(pad + along, edge), :], lane_shift(-across)))
        for t, tile in enumerate(pack_quad(rows, edge)):
            second_ref[:, (3 * quad + t) * LANES : (3 * quad + t + 1) * LANES] = tile


def at_group(pieces, refs, index):
    value = None
    for (_, start), ref in zip(pieces, refs):
        piece = ref[index]
        value = piece if value is None else jnp.where(pl.program_id(0) >= start, piece, value)
    return value


def combine_kernel(sizes, fields, folds, layout, *refs):
    scalars = Scalars(refs[:4], sizes)
    asked = refs[4]
    boxes_ref, before_ref, after_ref, low_ref, high_ref, *rest = refs[5:]
    out_ref, buffer, window = rest[-3:]
    field_refs = rest[:fields]
    rest = rest[fields:]
    by_slot = []
    for pieces in layout:
        slots = {}
        for piece, ref in zip(pieces, rest):
            slots.setdefault(piece[0], ([], []))
            slots[piece[0]][0].append(piece)
            slots[piece[0]][1].append(ref)
        by_slot.append(slots)
        rest = rest[len(pieces) :]
    firsts, seconds, early = by_slot
    orbital_count, _, edge, _ = boxes_ref.shape
    group = pl.program_id(0)
    last = pl.num_programs(0) - 1
    buffer[...] = jnp.zeros_like(buffer)
    position = 0
    planes = field_refs[0].shape[2]
    half = (fields - 1) // 2
    sources = [field_refs[:1]] + [(field_refs[1 + k], field_refs[1 + half + k]) for k in range(half)]
    for pair in sources:
        for s in range(pair[0].shape[0]):
            for y in range(GROUP):
                value = pair[0][s, y]
                for ref in pair[1:]:
                    value = value + ref[s, y]
                for copy in range(2**folds):
                    start = (position + copy * (REACH // 2**folds)) * planes
                    window[y, start : start + planes, :] = value
            position += 1

    def share(condition):
        return jnp.where(condition, FOCK_SHARE, 0.0)

    for orbital in range(orbital_count):
        begin = scalars.window_start(orbital)
        turn = lane_shift(-scalars.column(orbital))
        owned = scalars.position() * orbital_count + orbital
        for quad in range(GROUP // 4):
            rows = []
            for r in range(4):
                y = 4 * quad + r
                box = boxes_ref[orbital, y]
                if y == 0:
                    behind = jnp.where(group == 0, low_ref[orbital], before_ref[orbital, 0])
                else:
                    behind = boxes_ref[orbital, y - 1]
                if y == GROUP - 1:
                    ahead = jnp.where(group == last, high_ref[orbital], after_ref[orbital, 0])
                else:
                    ahead = boxes_ref[orbital, y + 1]
                buffer[y % 2, GROUP : GROUP + edge, :] = box
                beside = buffer[y % 2, GROUP - 1 : GROUP - 1 + edge, :]
                beside = beside + buffer[y % 2, GROUP + 1 : GROUP + 1 + edge, :]
                beside = beside + (behind + ahead)
                beside = beside + (roll_lanes(box, 1) + roll_lanes(box, LANES - 1))
                field = roll_lanes(window[y, pl.ds(begin, edge), :], turn)
                value = field * box - 0.5 * (beside - 6.0 * box)
                for slot, (pieces, held) in firsts.items():
                    scale = share(scalars.member(slot, 0) == orbital)
                    value = value - scale * at_group(pieces, held, y)
                rows.append(value)
            for t, tile in enumerate(pack_quad(rows, edge)):
                lanes = slice((3 * quad + t) * LANES, (3 * quad + t + 1) * LANES)
                for slot, (pieces, held) in seconds.items():
                    scale = share(scalars.member(slot, 1) == orbital)
                    tile = tile - scale * at_group(pieces, held, (slice(None), lanes))
                for slot, (pieces, held) in early.items():
                    scale = share(asked[slot, 1] == owned)
                    tile = tile - scale * at_group(pieces, held, (slice(None), lanes))
                out_ref[orbital, :, lanes] = tile


def finish_kernel(slot, starts, asked, ids, partial_ref, *refs):
    out_ref = refs[-1]
    orbital_count = partial_ref.shape[0]
    value = at_group([(slot, start) for start in starts], refs[:-1], Ellipsis)
    for orbital in range(orbital_count):
        mine = asked[slot, 1] == ids[0] * orbital_count + orbital
        out_ref[orbital] = partial_ref[orbital] - jnp.where(mine, FOCK_SHARE, 0.0) * value


def whole(shape):
    return pl.BlockSpec(shape, lambda g, *s: (0,) * len(shape))


def call(kernel, scalars, operands, in_specs, out_specs, out_shape, scratch, groups, flops):
    return pl.pallas_call(
        kernel,
        grid_spec=pltpu.PrefetchScalarGridSpec(
            num_scalar_prefetch=len(scalars),
            grid=(groups,),
            in_specs=in_specs,
            out_specs=out_specs,
            scratch_shapes=scratch,
        ),
        out_shape=out_shape,
        cost_estimate=pl.CostEstimate(
            flops=flops, bytes_accessed=4_000_000, transcendentals=0
        ),
        compiler_params=pltpu.CompilerParams(
            dimension_semantics=("arbitrary",), vmem_limit_bytes=VMEM_LIMIT
        ),
    )(*scalars, *operands)


def program(orbitals, external_potential, corners, pair_list, pair_count):
    f32 = jnp.float32
    orbital_count, edge, merged = orbitals.shape
    rows = merged // edge
    groups = rows // GROUP
    lanes = GROUP * edge
    devices = lax.axis_size("slab")
    sub_count = lax.axis_size("sub")
    position = lax.axis_index("slab")
    place = lax.axis_index("sub")
    plane_count = external_potential.shape[0]
    grid_planes = plane_count * devices
    sizes = (orbital_count, plane_count, grid_planes)
    spread = REACH * plane_count - edge
    pad = spread + plane_count
    slot_count = pair_list.shape[0]
    kept = edge * edge // LANES
    chunk = kept // sub_count * GROUP
    folds = 0
    while (REACH >> (folds + 1)) >= 2 and (REACH >> (folds + 1)) % devices == 0:
        folds += 1
    slabs = REACH >> folds
    padded, stacked = (jnp.asarray(t) for t in sine_tables(edge))
    columns, own_levels = (jnp.asarray(t) for t in level_tables(edge))
    flops = 200_000_000
    ids = jnp.stack([position, place]).astype(jnp.int32)
    scalars = (corners, pair_list, pair_count, ids)

    asked = from_behind(pair_list, "slab", 1)

    box_shape = (orbital_count, rows, edge, LANES)
    own_spec = pl.BlockSpec((orbital_count, edge, lanes), lambda g, *s: (0, 0, g))
    windows = call(
        functools.partial(spread_kernel, sizes, folds),
        (corners, ids),
        (orbitals,),
        [own_spec],
        [pl.BlockSpec((2, GROUP, plane_count, LANES), lambda g, *s: (0, g, 0, 0))] * (slabs // 2),
        [jax.ShapeDtypeStruct((2, rows, plane_count, LANES), f32)] * (slabs // 2),
        [pltpu.VMEM((orbital_count, GROUP, edge + 2 * spread, LANES), f32)],
        groups,
        flops,
    )
    boxes = call(
        unpack_kernel,
        (),
        (orbitals,),
        [own_spec],
        [pl.BlockSpec((orbital_count, GROUP, edge, LANES), lambda g, *s: (0, g, 0, 0))],
        [jax.ShapeDtypeStruct(box_shape, f32)],
        [],
        groups,
        flops,
    )[0]

    near = windows[0]
    parts = []
    for hop in range(2, slabs, 2):
        parts.append(from_behind(windows[hop // 2], "slab", hop))
    for part in parts:
        near = near + part
    onward = from_behind(near[1], "slab", 1)
    density = (near[0] + onward).transpose(1, 0, 2).reshape(external_potential.shape)
    local_field = external_potential - LOCAL_FACTOR * jnp.cbrt(density + EPSILON)
    local_field = local_field.reshape(plane_count, rows, LANES).transpose(1, 0, 2)
    beyond = from_behind(local_field, "slab", -1)
    both = jnp.stack([local_field, beyond])
    fields = [both]
    for parity in (1, 0):
        for hop in range(2, slabs, 2):
            pairs = [(i, (i - hop) % devices) for i in range(parity, devices, 2)]
            fields.append(lax.ppermute(both, "slab", pairs))

    answers = []
    for k in range(slot_count):
        picked = lax.dynamic_index_in_dim(
            orbitals, lax.rem(asked[k, 1], orbital_count), 0, keepdims=False
        )
        answers.append(from_behind(picked, "slab", -1))

    forward = [(i, i + 1) for i in range(sub_count - 1)]
    backward = [(target, source) for source, target in forward]
    low_halo = lax.ppermute(boxes[:, rows - 1], "sub", forward)
    high_halo = lax.ppermute(boxes[:, 0], "sub", backward)

    def side(slot, pick, start=0):
        def index(g, c, p, n, d):
            scalar = Scalars((c, p, n, d), sizes)
            return (scalar.kept(slot) if pick else scalar.member(slot, 0), g + start, 0, 0)

        return pl.BlockSpec((1, GROUP, edge, LANES), index)

    row_spec = pl.BlockSpec((GROUP, edge, LANES), lambda g, *s: (g, 0, 0))
    dense_spec = pl.BlockSpec((edge, lanes), lambda g, *s: (0, g))
    piece_spec = pl.BlockSpec((1, chunk, LANES), lambda g, *s: (g, 0, 0))
    piece_shape = jax.ShapeDtypeStruct((groups, chunk, LANES), f32)
    shifted = pltpu.VMEM((GROUP, edge + 2 * pad, LANES), f32)
    flat = pltpu.VMEM((kept * GROUP, LANES), f32)
    solve_steps = 3
    tall = chunk // solve_steps
    tall_spec = pl.BlockSpec((groups, tall, LANES), lambda g, *s: (0, g, 0))
    firsts, seconds, returns = [], [], []
    for slot in range(slot_count):
        outs = call(
            functools.partial(forward_kernel, sizes, sub_count, pad, slot),
            scalars,
            (boxes, boxes, answers[slot], padded, stacked),
            [side(slot, 0), side(slot, 1), dense_spec, whole(padded.shape), whole(stacked.shape)],
            [piece_spec] * sub_count + [row_spec],
            [piece_shape] * sub_count + [jax.ShapeDtypeStruct((rows, edge, LANES), f32)],
            [shifted, flat],
            groups,
            flops,
        )
        moved = outs[sub_count]
        pieces = exchange(outs[:sub_count], "sub")
        final = slot == slot_count - 1
        parts = [(0, 1), (1, groups - 1)] if final and groups > 1 else [(0, groups)]
        solved = call(
            functools.partial(solve_kernel, sizes, sub_count, groups, parts),
            scalars,
            (*pieces, columns, own_levels, stacked),
            [tall_spec] * sub_count
            + [whole(columns.shape), whole(own_levels.shape), whole(stacked.shape)],
            [
                pl.BlockSpec((count, tall, LANES), lambda g, *s: (0, g, 0))
                for _, count in parts
                for _ in range(sub_count)
            ],
            [
                jax.ShapeDtypeStruct((count, chunk, LANES), f32)
                for _, count in parts
                for _ in range(sub_count)
            ],
            [pltpu.VMEM((tall // GROUP // 2, edge, 2 * LANES), f32)],
            solve_steps,
            flops,
        )
        received = [
            exchange(solved[part * sub_count : (part + 1) * sub_count], "sub")
            for part in range(len(parts))
        ]
        for part, (start, count) in enumerate(parts):
            first, second = call(
                functools.partial(backward_kernel, sizes, sub_count, pad, slot),
                scalars,
                (*received[part], boxes, moved, padded, stacked),
                [piece_spec] * sub_count
                + [
                    side(slot, 0, start),
                    pl.BlockSpec(
                        (GROUP, edge, LANES), lambda g, *s, start=start: (g + start, 0, 0)
                    ),
                    whole(padded.shape),
                    whole(stacked.shape),
                ],
                [row_spec, dense_spec],
                [
                    jax.ShapeDtypeStruct((count * GROUP, edge, LANES), f32),
                    jax.ShapeDtypeStruct((edge, count * lanes), f32),
                ],
                [shifted, flat],
                count,
                flops * count // groups,
            )
            firsts.append((slot, start, count, first))
            seconds.append((slot, start, count, second))
            returns.append((slot, start, count, from_behind(second, "slab", 1)))

    def group_spec(shape, axis, start, count):
        def index(g, *s):
            at = [0] * len(shape)
            at[axis] = jnp.clip(g - start, 0, count - 1)
            return tuple(at)

        return pl.BlockSpec(shape, index)

    early = [r for r in returns if r[0] < slot_count - 1]
    late = [r for r in returns if r[0] == slot_count - 1]
    layout = [
        [(slot, start) for slot, start, _, _ in pieces] for pieces in (firsts, seconds, early)
    ]
    edge_block = (orbital_count, 1, edge, LANES)
    partial = call(
        functools.partial(combine_kernel, sizes, len(fields), folds, layout),
        (*scalars, asked),
        (
            boxes,
            boxes,
            boxes,
            low_halo,
            high_halo,
            *fields,
            *(piece for pieces in (firsts, seconds, early) for *_, piece in pieces),
        ),
        [
            pl.BlockSpec((orbital_count, GROUP, edge, LANES), lambda g, *s: (0, g, 0, 0)),
            pl.BlockSpec(edge_block, lambda g, *s: (0, jnp.maximum(g * GROUP - 1, 0), 0, 0)),
            pl.BlockSpec(
                edge_block, lambda g, *s: (0, jnp.minimum((g + 1) * GROUP, rows - 1), 0, 0)
            ),
            whole((orbital_count, edge, LANES)),
            whole((orbital_count, edge, LANES)),
        ]
        + [
            pl.BlockSpec((f.shape[0], GROUP, plane_count, LANES), lambda g, *s: (0, g, 0, 0))
            for f in fields
        ]
        + [group_spec((GROUP, edge, LANES), 0, start, count) for _, start, count, _ in firsts]
        + [
            group_spec((edge, lanes), 1, start, count)
            for pieces in (seconds, early)
            for _, start, count, _ in pieces
        ],
        [pl.BlockSpec((orbital_count, edge, lanes), lambda g, *s: (0, 0, g))],
        [jax.ShapeDtypeStruct(orbitals.shape, f32)],
        [
            pltpu.VMEM((2, edge + 2 * GROUP, LANES), f32),
            pltpu.VMEM((GROUP, REACH * plane_count, LANES), f32),
        ],
        groups,
        flops,
    )[0]

    return call(
        functools.partial(finish_kernel, slot_count - 1, [start for _, start, _, _ in late]),
        (asked, ids),
        (partial, *(piece for *_, piece in late)),
        [own_spec] + [group_spec((edge, lanes), 1, start, count) for _, start, count, _ in late],
        [own_spec],
        [jax.ShapeDtypeStruct(orbitals.shape, f32)],
        [],
        groups,
        flops,
    )[0]


def solution(mesh):
    placed = (P("slab", None, "sub"), P("slab", "sub"), P(), P("slab", None), P("slab"))
    return jax.shard_map(
        program, mesh=mesh, in_specs=placed, out_specs=P("slab", None, "sub"), check_vma=False
    )
```

```python
import functools
import math

import jax
import jax.numpy as jnp
import numpy as np
from jax import lax
from jax.experimental import pallas as pl
from jax.experimental.pallas import tpu as pltpu
from jax.sharding import PartitionSpec as P

REACH = 16
LANES = 128
GROUP = 8
VMEM_LIMIT = 20 << 20

SCREEN = 0.0008
FOCK_SHARE = 0.25
LOCAL_FACTOR = (3.0 / math.pi) ** (1.0 / 3.0)
EPSILON = 1e-06


def from_behind(value, axis, by):
    size = lax.axis_size(axis)
    return lax.ppermute(value, axis, [(i, (i + by) % size) for i in range(size)])


def partner(index, step, size):
    if size & (size - 1) == 0:
        return index ^ step
    return (size - index + step) % size


def exchange(pieces, axis):
    size = lax.axis_size(axis)
    received = []
    for step, piece in enumerate(pieces):
        pairs = [(i, partner(i, step, size)) for i in range(size)]
        if all(source == target for source, target in pairs):
            received.append(piece)
        else:
            received.append(lax.ppermute(piece, axis, pairs))
    return received


def split_bf16(value):
    high = value.astype(jnp.bfloat16)
    low = (value - high.astype(jnp.float32)).astype(jnp.bfloat16)
    return high, low


def sine_tables(box_edge):
    levels = np.arange(1, box_edge + 1, dtype=np.float64)
    sine = np.sqrt(2.0 / (box_edge + 1)) * np.sin(
        np.pi * levels[:, None] * levels[None, :] / (box_edge + 1)
    )
    sine = sine.astype(np.float32)
    high = sine.astype(jnp.bfloat16)
    low = (sine - high.astype(np.float32)).astype(jnp.bfloat16)
    padded = np.zeros((LANES, 2 * LANES), dtype=high.dtype)
    padded[:box_edge, :box_edge] = high
    padded[:box_edge, LANES : LANES + box_edge] = low
    stacked = np.concatenate([high, low], axis=0)
    return padded, stacked


def level_tables(box_edge):
    levels = np.arange(1, box_edge + 1, dtype=np.float64)
    levels = 2.0 - 2.0 * np.cos(np.pi * levels / (box_edge + 1))
    kept = box_edge * box_edge // LANES
    spare = LANES - box_edge
    low_rows = box_edge - kept
    columns = np.zeros((kept, LANES), np.float64)
    for row in range(kept):
        columns[row, :box_edge] = levels[row] + levels
        part = row // low_rows
        columns[row, box_edge:] = (
            levels[kept + row % low_rows] + levels[part * spare : (part + 1) * spare]
        )
    own = np.repeat(levels[:, None], 2 * LANES, axis=1)
    return columns.astype(np.float32), own.astype(np.float32)


def lane_index(shape):
    return lax.broadcasted_iota(jnp.int32, shape, len(shape) - 1)


def roll_lanes(value, shift):
    return pltpu.roll(value, shift, 1)


def unpack_quad(tiles, edge):
    first, second, third = tiles
    lane = lane_index(first.shape)
    spare = LANES - edge
    keep = lane < edge
    rows = [
        first,
        roll_lanes(jnp.where(lane >= edge, first, second), spare),
        roll_lanes(jnp.where(lane >= edge - spare, second, third), 2 * spare),
        roll_lanes(third, 3 * spare),
    ]
    return [jnp.where(keep, row, 0.0) for row in rows]


def pack_quad(rows, edge):
    zero, one, two, three = rows
    lane = lane_index(zero.shape)
    spare = LANES - edge
    one = roll_lanes(one, edge)
    two = roll_lanes(two, edge - spare)
    three = roll_lanes(three, spare)
    return [
        jnp.where(lane < edge, zero, one),
        jnp.where(lane < edge - spare, one, two),
        jnp.where(lane < spare, two, three),
    ]


def transform_lanes(value, padded_ref):
    high, low = split_bf16(value)
    both = jnp.dot(high, padded_ref[...], preferred_element_type=jnp.float32)
    rest = jnp.dot(low, padded_ref[:, :LANES], preferred_element_type=jnp.float32)
    return both[:, :LANES] + (both[:, LANES:] + rest)


def transform_rows(value, stacked_ref):
    edge = stacked_ref.shape[0] // 2
    high, low = split_bf16(value)
    both = jnp.dot(stacked_ref[...], high, preferred_element_type=jnp.float32)
    rest = jnp.dot(stacked_ref[:edge, :], low, preferred_element_type=jnp.float32)
    return both[:edge] + (both[edge:] + rest)


class Scalars:
    def __init__(self, refs, sizes):
        self.corners, self.pairs, self.count, self.ids = refs
        self.orbital_count, self.plane_count, self.grid_planes = sizes
        self.total = self.corners.shape[0]

    def position(self):
        return self.ids[0]

    def place(self):
        return self.ids[1]

    def window_start(self, orbital):
        first = self.corners[self.position() * self.orbital_count + orbital, 0]
        return lax.rem(
            first - self.position() * self.plane_count + self.grid_planes, self.grid_planes
        )

    def column(self, orbital):
        return self.corners[self.position() * self.orbital_count + orbital, 1]

    def member(self, slot, side):
        owned = self.pairs[slot, side] - self.position() * self.orbital_count
        return lax.rem(owned + self.total, self.total)

    def remote(self, slot):
        return self.member(slot, 1) >= self.orbital_count

    def kept(self, slot):
        return jnp.minimum(self.member(slot, 1), self.orbital_count - 1)

    def shifts(self, slot):
        first, second = self.pairs[slot, 0], self.pairs[slot, 1]
        half = self.grid_planes // 2
        along = self.corners[second, 0] - self.corners[first, 0] + half + self.grid_planes
        return (
            lax.rem(along, self.grid_planes) - half,
            self.corners[second, 1] - self.corners[first, 1],
        )

    def weight(self, slot):
        return jnp.where(slot < self.count[0], 1.0, 0.0).astype(jnp.float32)


def lane_shift(amount):
    return lax.rem(amount + LANES, LANES)


def spread_kernel(sizes, folds, corners, ids, dense_ref, *refs):
    scalars = Scalars((corners, None, None, ids), sizes)
    *window_refs, buffer = refs
    orbital_count, edge, _ = dense_ref.shape
    planes = window_refs[0].shape[2]
    window_planes = REACH * planes
    spread = window_planes - edge

    @pl.when(pl.program_id(0) == 0)
    def _():
        buffer[:, :, :spread, :] = jnp.zeros_like(buffer[:, :, :spread, :])
        buffer[:, :, spread + edge :, :] = jnp.zeros_like(buffer[:, :, spread + edge :, :])

    for orbital in range(orbital_count):
        for quad in range(GROUP // 4):
            tiles = [
                dense_ref[orbital, :, (3 * quad + t) * LANES : (3 * quad + t + 1) * LANES]
                for t in range(3)
            ]
            for r, row in enumerate(unpack_quad(tiles, edge)):
                buffer[orbital, 4 * quad + r, spread : spread + edge, :] = roll_lanes(
                    row * row, scalars.column(orbital)
                )
    for y in range(GROUP):
        total = None
        for orbital in range(orbital_count):
            start = spread - scalars.window_start(orbital)
            placed = buffer[orbital, y, pl.ds(start, window_planes), :]
            total = placed if total is None else total + placed
        for _ in range(folds):
            half = total.shape[0] // 2
            total = total[:half] + total[half:]
        for s in range(2 * len(window_refs)):
            window_refs[s // 2][s % 2, y] = total[s * planes : (s + 1) * planes]


def unpack_kernel(dense_ref, boxes_ref):
    orbital_count, edge, _ = dense_ref.shape
    for orbital in range(orbital_count):
        for quad in range(GROUP // 4):
            tiles = [
                dense_ref[orbital, :, (3 * quad + t) * LANES : (3 * quad + t + 1) * LANES]
                for t in range(3)
            ]
            for r, row in enumerate(unpack_quad(tiles, edge)):
                boxes_ref[orbital, 4 * quad + r] = row


def forward_kernel(sizes, sub_count, pad, slot, *refs):
    scalars = Scalars(refs[:4], sizes)
    own_ref, second_ref, dense_ref, padded_ref, stacked_ref = refs[4:9]
    outs = refs[9 : 9 + sub_count]
    moved_ref, buffer, flat = refs[9 + sub_count :]
    edge = own_ref.shape[2]
    remote = scalars.remote(slot)

    @pl.when(pl.program_id(0) == 0)
    def _():
        buffer[:, :pad, :] = jnp.zeros((GROUP, pad, LANES), jnp.float32)
        buffer[:, pad + edge :, :] = jnp.zeros((GROUP, pad, LANES), jnp.float32)

    @pl.when(remote)
    def _():
        for quad in range(GROUP // 4):
            tiles = [
                dense_ref[:, (3 * quad + t) * LANES : (3 * quad + t + 1) * LANES]
                for t in range(3)
            ]
            for r, row in enumerate(unpack_quad(tiles, edge)):
                buffer[4 * quad + r, pad : pad + edge, :] = row

    @pl.when(jnp.logical_not(remote))
    def _():
        buffer[:, pad : pad + edge, :] = second_ref[0]

    along, across = scalars.shifts(slot)
    lane = lane_index((edge, LANES))
    products = []
    for y in range(GROUP):
        moved = roll_lanes(buffer[y, pl.ds(pad - along, edge), :], lane_shift(across))
        moved = jnp.where(lane < edge, moved, 0.0)
        moved_ref[y] = moved
        products.append(own_ref[0, y] * moved)
    turned = transform_lanes(jnp.concatenate(products, axis=0), padded_ref)
    kept = edge * edge // LANES
    low_rows = edge - kept
    spare = LANES - edge
    keep = lane_index((kept, LANES)) < edge
    for y in range(0, GROUP, 2):
        pair = jnp.concatenate(
            [turned[(y + k) * edge : (y + k + 1) * edge] for k in range(2)], axis=1
        )
        pair = transform_rows(pair, stacked_ref)
        for k in range(2):
            spectral = pair[:, k * LANES : (k + 1) * LANES]
            low = spectral[kept:]
            tail = jnp.concatenate(
                [roll_lanes(low, edge - part * spare) for part in range(kept // low_rows)], axis=0
            )
            flat[pl.ds(y + k, kept, stride=GROUP), :] = jnp.where(keep, spectral[:kept], tail)
    chunk = kept // sub_count * GROUP
    for step in range(sub_count):
        target = partner(scalars.place(), step, sub_count)
        outs[step][0] = flat[pl.ds(pl.multiple_of(target * chunk, GROUP), chunk), :]


def solve_kernel(sizes, sub_count, inward, outward, *refs):
    scalars = Scalars(refs[:4], sizes)
    rest = refs[4:]
    pieces = rest[: len(inward) * sub_count]
    columns_ref, levels_ref, stacked_ref, *outs, work = rest[len(inward) * sub_count :]
    count = pieces[0].shape[1] // GROUP
    edge = stacked_ref.shape[0] // 2
    rows = edge // sub_count
    for part, (first_group, group_count) in enumerate(inward):
        for step in range(sub_count):
            source = partner(scalars.place(), step, sub_count)
            piece = pieces[part * sub_count + step]
            for g in range(group_count):
                base = pl.multiple_of(source * rows + (first_group + g) * GROUP, GROUP)
                for q in range(count):
                    work[q // 2, pl.ds(base, GROUP), (q % 2) * LANES : (q % 2 + 1) * LANES] = piece[
                        g, q * GROUP : (q + 1) * GROUP, :
                    ]
    first = scalars.place() * (count * pl.num_programs(0)) + pl.program_id(0) * count
    for pair in range(count // 2):
        spectral = transform_rows(work[pair], stacked_ref)
        column = jnp.concatenate(
            [columns_ref[pl.ds(first + 2 * pair + k, 1), :] for k in range(2)], axis=1
        )
        spectral = spectral * ((4.0 * math.pi) / (levels_ref[...] + column + SCREEN))
        work[pair] = transform_rows(spectral, stacked_ref)
    for step in range(sub_count):
        target = partner(scalars.place(), step, sub_count)
        for part, (first_group, group_count) in enumerate(outward):
            out = outs[part * sub_count + step]
            for g in range(group_count):
                base = pl.multiple_of(target * rows + (first_group + g) * GROUP, GROUP)
                for q in range(count):
                    out[g, q * GROUP : (q + 1) * GROUP, :] = work[
                        q // 2, pl.ds(base, GROUP), (q % 2) * LANES : (q % 2 + 1) * LANES
                    ]


def backward_kernel(sizes, sub_count, pad, slot, *refs):
    scalars = Scalars(refs[:4], sizes)
    rest = refs[4:]
    pieces = rest[:sub_count]
    own_ref, moved_ref, padded_ref, stacked_ref, first_ref, second_ref, buffer, flat = rest[
        sub_count:
    ]
    edge = own_ref.shape[2]
    weight = scalars.weight(slot)
    kept = edge * edge // LANES
    low_rows = edge - kept
    spare = LANES - edge
    chunk = kept // sub_count * GROUP

    @pl.when(pl.program_id(0) == 0)
    def _():
        buffer[:, :pad, :] = jnp.zeros((GROUP, pad, LANES), jnp.float32)
        buffer[:, pad + edge :, :] = jnp.zeros((GROUP, pad, LANES), jnp.float32)

    for step in range(sub_count):
        source = partner(scalars.place(), step, sub_count)
        flat[pl.ds(pl.multiple_of(source * chunk, GROUP), chunk), :] = pieces[step][0]
    lane = lane_index((low_rows, LANES))
    turned = []
    for y in range(0, GROUP, 2):
        pair = []
        for k in range(2):
            packed = flat[pl.ds(y + k, kept, stride=GROUP), :]
            low = None
            for part in range(kept // low_rows - 1, -1, -1):
                piece = roll_lanes(
                    packed[part * low_rows : (part + 1) * low_rows], (part + 1) * spare
                )
                low = piece if low is None else jnp.where(lane < (part + 1) * spare, piece, low)
            pair.append(jnp.concatenate([packed, low], axis=0))
        pair = transform_rows(jnp.concatenate(pair, axis=1), stacked_ref)
        turned += [pair[:, :LANES], pair[:, LANES:]]
    potential = transform_lanes(jnp.concatenate(turned, axis=0), padded_ref)
    along, across = scalars.shifts(slot)
    for quad in range(GROUP // 4):
        rows = []
        for r in range(4):
            y = 4 * quad + r
            solved = potential[y * edge : (y + 1) * edge] * weight
            first_ref[y] = solved * moved_ref[y]
            buffer[y, pad : pad + edge, :] = solved * own_ref[0, y]
            rows.append(roll_lanes(buffer[y, pl.ds(pad + along, edge), :], lane_shift(-across)))
        for t, tile in enumerate(pack_quad(rows, edge)):
            second_ref[:, (3 * quad + t) * LANES : (3 * quad + t + 1) * LANES] = tile


def at_group(pieces, refs, index):
    value = None
    for (_, start), ref in zip(pieces, refs):
        piece = ref[index]
        value = piece if value is None else jnp.where(pl.program_id(0) >= start, piece, value)
    return value


def combine_kernel(sizes, fields, folds, layout, *refs):
    scalars = Scalars(refs[:4], sizes)
    asked = refs[4]
    boxes_ref, before_ref, after_ref, low_ref, high_ref, *rest = refs[5:]
    out_ref, buffer, window = rest[-3:]
    field_refs = rest[:fields]
    rest = rest[fields:]
    by_slot = []
    for pieces in layout:
        slots = {}
        for piece, ref in zip(pieces, rest):
            slots.setdefault(piece[0], ([], []))
            slots[piece[0]][0].append(piece)
            slots[piece[0]][1].append(ref)
        by_slot.append(slots)
        rest = rest[len(pieces) :]
    firsts, seconds, early = by_slot
    orbital_count, _, edge, _ = boxes_ref.shape
    group = pl.program_id(0)
    last = pl.num_programs(0) - 1
    buffer[...] = jnp.zeros_like(buffer)
    position = 0
    planes = field_refs[0].shape[2]
    half = (fields - 1) // 2
    sources = [field_refs[:1]] + [(field_refs[1 + k], field_refs[1 + half + k]) for k in range(half)]
    for pair in sources:
        for s in range(pair[0].shape[0]):
            for y in range(GROUP):
                value = pair[0][s, y]
                for ref in pair[1:]:
                    value = value + ref[s, y]
                for copy in range(2**folds):
                    start = (position + copy * (REACH // 2**folds)) * planes
                    window[y, start : start + planes, :] = value
            position += 1

    def share(condition):
        return jnp.where(condition, FOCK_SHARE, 0.0)

    for orbital in range(orbital_count):
        begin = scalars.window_start(orbital)
        turn = lane_shift(-scalars.column(orbital))
        owned = scalars.position() * orbital_count + orbital
        for quad in range(GROUP // 4):
            rows = []
            for r in range(4):
                y = 4 * quad + r
                box = boxes_ref[orbital, y]
                if y == 0:
                    behind = jnp.where(group == 0, low_ref[orbital], before_ref[orbital, 0])
                else:
                    behind = boxes_ref[orbital, y - 1]
                if y == GROUP - 1:
                    ahead = jnp.where(group == last, high_ref[orbital], after_ref[orbital, 0])
                else:
                    ahead = boxes_ref[orbital, y + 1]
                buffer[y % 2, GROUP : GROUP + edge, :] = box
                beside = buffer[y % 2, GROUP - 1 : GROUP - 1 + edge, :]
                beside = beside + buffer[y % 2, GROUP + 1 : GROUP + 1 + edge, :]
                beside = beside + (behind + ahead)
                beside = beside + (roll_lanes(box, 1) + roll_lanes(box, LANES - 1))
                field = roll_lanes(window[y, pl.ds(begin, edge), :], turn)
                value = field * box - 0.5 * (beside - 6.0 * box)
                for slot, (pieces, held) in firsts.items():
                    scale = share(scalars.member(slot, 0) == orbital)
                    value = value - scale * at_group(pieces, held, y)
                rows.append(value)
            for t, tile in enumerate(pack_quad(rows, edge)):
                lanes = slice((3 * quad + t) * LANES, (3 * quad + t + 1) * LANES)
                for slot, (pieces, held) in seconds.items():
                    scale = share(scalars.member(slot, 1) == orbital)
                    tile = tile - scale * at_group(pieces, held, (slice(None), lanes))
                for slot, (pieces, held) in early.items():
                    scale = share(asked[slot, 1] == owned)
                    tile = tile - scale * at_group(pieces, held, (slice(None), lanes))
                out_ref[orbital, :, lanes] = tile


def finish_kernel(slot, starts, asked, ids, partial_ref, *refs):
    out_ref = refs[-1]
    orbital_count = partial_ref.shape[0]
    value = at_group([(slot, start) for start in starts], refs[:-1], Ellipsis)
    for orbital in range(orbital_count):
        mine = asked[slot, 1] == ids[0] * orbital_count + orbital
        out_ref[orbital] = partial_ref[orbital] - jnp.where(mine, FOCK_SHARE, 0.0) * value


def whole(shape):
    return pl.BlockSpec(shape, lambda g, *s: (0,) * len(shape))


def call(kernel, scalars, operands, in_specs, out_specs, out_shape, scratch, groups, flops):
    return pl.pallas_call(
        kernel,
        grid_spec=pltpu.PrefetchScalarGridSpec(
            num_scalar_prefetch=len(scalars),
            grid=(groups,),
            in_specs=in_specs,
            out_specs=out_specs,
            scratch_shapes=scratch,
        ),
        out_shape=out_shape,
        cost_estimate=pl.CostEstimate(
            flops=flops, bytes_accessed=4_000_000, transcendentals=0
        ),
        compiler_params=pltpu.CompilerParams(
            dimension_semantics=("arbitrary",), vmem_limit_bytes=VMEM_LIMIT
        ),
    )(*scalars, *operands)


def program(orbitals, external_potential, corners, pair_list, pair_count):
    f32 = jnp.float32
    orbital_count, edge, merged = orbitals.shape
    rows = merged // edge
    groups = rows // GROUP
    lanes = GROUP * edge
    devices = lax.axis_size("slab")
    sub_count = lax.axis_size("sub")
    position = lax.axis_index("slab")
    place = lax.axis_index("sub")
    plane_count = external_potential.shape[0]
    grid_planes = plane_count * devices
    sizes = (orbital_count, plane_count, grid_planes)
    spread = REACH * plane_count - edge
    pad = spread + plane_count
    slot_count = pair_list.shape[0]
    kept = edge * edge // LANES
    chunk = kept // sub_count * GROUP
    folds = 0
    while (REACH >> (folds + 1)) >= 2 and (REACH >> (folds + 1)) % devices == 0:
        folds += 1
    slabs = REACH >> folds
    padded, stacked = (jnp.asarray(t) for t in sine_tables(edge))
    columns, own_levels = (jnp.asarray(t) for t in level_tables(edge))
    flops = 200_000_000
    ids = jnp.stack([position, place]).astype(jnp.int32)
    scalars = (corners, pair_list, pair_count, ids)

    asked = from_behind(pair_list, "slab", 1)

    box_shape = (orbital_count, rows, edge, LANES)
    own_spec = pl.BlockSpec((orbital_count, edge, lanes), lambda g, *s: (0, 0, g))
    windows = call(
        functools.partial(spread_kernel, sizes, folds),
        (corners, ids),
        (orbitals,),
        [own_spec],
        [pl.BlockSpec((2, GROUP, plane_count, LANES), lambda g, *s: (0, g, 0, 0))] * (slabs // 2),
        [jax.ShapeDtypeStruct((2, rows, plane_count, LANES), f32)] * (slabs // 2),
        [pltpu.VMEM((orbital_count, GROUP, edge + 2 * spread, LANES), f32)],
        groups,
        flops,
    )
    boxes = call(
        unpack_kernel,
        (),
        (orbitals,),
        [own_spec],
        [pl.BlockSpec((orbital_count, GROUP, edge, LANES), lambda g, *s: (0, g, 0, 0))],
        [jax.ShapeDtypeStruct(box_shape, f32)],
        [],
        groups,
        flops,
    )[0]

    near = windows[0]
    parts = []
    for hop in range(2, slabs, 2):
        parts.append(from_behind(windows[hop // 2], "slab", hop))
    for part in parts:
        near = near + part
    onward = from_behind(near[1], "slab", 1)
    density = (near[0] + onward).transpose(1, 0, 2).reshape(external_potential.shape)
    local_field = external_potential - LOCAL_FACTOR * jnp.cbrt(density + EPSILON)
    local_field = local_field.reshape(plane_count, rows, LANES).transpose(1, 0, 2)
    beyond = from_behind(local_field, "slab", -1)
    both = jnp.stack([local_field, beyond])
    fields = [both]
    for parity in (1, 0):
        for hop in range(2, slabs, 2):
            pairs = [(i, (i - hop) % devices) for i in range(parity, devices, 2)]
            fields.append(lax.ppermute(both, "slab", pairs))

    answers = []
    for k in range(slot_count):
        picked = lax.dynamic_index_in_dim(
            orbitals, lax.rem(asked[k, 1], orbital_count), 0, keepdims=False
        )
        answers.append(from_behind(picked, "slab", -1))

    forward = [(i, i + 1) for i in range(sub_count - 1)]
    backward = [(target, source) for source, target in forward]
    low_halo = lax.ppermute(boxes[:, rows - 1], "sub", forward)
    high_halo = lax.ppermute(boxes[:, 0], "sub", backward)

    def side(slot, pick, start=0):
        def index(g, c, p, n, d):
            scalar = Scalars((c, p, n, d), sizes)
            return (scalar.kept(slot) if pick else scalar.member(slot, 0), g + start, 0, 0)

        return pl.BlockSpec((1, GROUP, edge, LANES), index)

    row_spec = pl.BlockSpec((GROUP, edge, LANES), lambda g, *s: (g, 0, 0))
    dense_spec = pl.BlockSpec((edge, lanes), lambda g, *s: (0, g))
    piece_spec = pl.BlockSpec((1, chunk, LANES), lambda g, *s: (g, 0, 0))
    shifted = pltpu.VMEM((GROUP, edge + 2 * pad, LANES), f32)
    flat = pltpu.VMEM((kept * GROUP, LANES), f32)
    solve_steps = 3
    tall = chunk // solve_steps
    tall_spec = pl.BlockSpec((groups, tall, LANES), lambda g, *s: (0, g, 0))
    firsts, seconds, returns = [], [], []
    pieced = [(0, 1), (1, groups - 1)] if groups > 1 else [(0, groups)]

    def tall_specs(parts):
        return [
            pl.BlockSpec((count, tall, LANES), lambda g, *s: (0, g, 0))
            for _, count in parts
            for _ in range(sub_count)
        ]

    def rows_from(start):
        return pl.BlockSpec((GROUP, edge, LANES), lambda g, *s: (g + start, 0, 0))

    for slot in range(slot_count):
        inward = [(0, groups)]
        pieces = []
        moved = {}
        for start, count in inward:
            outs = call(
                functools.partial(forward_kernel, sizes, sub_count, pad, slot),
                scalars,
                (boxes, boxes, answers[slot], padded, stacked),
                [
                    side(slot, 0, start),
                    side(slot, 1, start),
                    pl.BlockSpec((edge, lanes), lambda g, *s, start=start: (0, g + start)),
                    whole(padded.shape),
                    whole(stacked.shape),
                ],
                [piece_spec] * sub_count + [row_spec],
                [jax.ShapeDtypeStruct((count, chunk, LANES), f32)] * sub_count
                + [jax.ShapeDtypeStruct((count * GROUP, edge, LANES), f32)],
                [shifted, flat],
                count,
                flops * count // groups,
            )
            moved[start] = outs[sub_count]
            pieces += exchange(outs[:sub_count], "sub")
        outward = pieced
        solved = call(
            functools.partial(solve_kernel, sizes, sub_count, inward, outward),
            scalars,
            (*pieces, columns, own_levels, stacked),
            tall_specs(inward)
            + [whole(columns.shape), whole(own_levels.shape), whole(stacked.shape)],
            tall_specs(outward),
            [
                jax.ShapeDtypeStruct((count, chunk, LANES), f32)
                for _, count in outward
                for _ in range(sub_count)
            ],
            [pltpu.VMEM((tall // GROUP // 2, edge, 2 * LANES), f32)],
            solve_steps,
            flops,
        )
        received = [
            exchange(solved[part * sub_count : (part + 1) * sub_count], "sub")
            for part in range(len(outward))
        ]
        for part, (start, count) in enumerate(outward):
            origin = max(first for first in moved if first <= start)
            first, second = call(
                functools.partial(backward_kernel, sizes, sub_count, pad, slot),
                scalars,
                (*received[part], boxes, moved[origin], padded, stacked),
                [piece_spec] * sub_count
                + [
                    side(slot, 0, start),
                    rows_from(start - origin),
                    whole(padded.shape),
                    whole(stacked.shape),
                ],
                [row_spec, dense_spec],
                [
                    jax.ShapeDtypeStruct((count * GROUP, edge, LANES), f32),
                    jax.ShapeDtypeStruct((edge, count * lanes), f32),
                ],
                [shifted, flat],
                count,
                flops * count // groups,
            )
            firsts.append((slot, start, count, first))
            seconds.append((slot, start, count, second))
            returns.append((slot, start, count, from_behind(second, "slab", 1)))

    def group_spec(shape, axis, start, count):
        def index(g, *s):
            at = [0] * len(shape)
            at[axis] = jnp.clip(g - start, 0, count - 1)
            return tuple(at)

        return pl.BlockSpec(shape, index)

    early = [r for r in returns if r[0] < slot_count - 1]
    late = [r for r in returns if r[0] == slot_count - 1]
    layout = [
        [(slot, start) for slot, start, _, _ in pieces] for pieces in (firsts, seconds, early)
    ]
    edge_block = (orbital_count, 1, edge, LANES)
    partial = call(
        functools.partial(combine_kernel, sizes, len(fields), folds, layout),
        (*scalars, asked),
        (
            boxes,
            boxes,
            boxes,
            low_halo,
            high_halo,
            *fields,
            *(piece for pieces in (firsts, seconds, early) for *_, piece in pieces),
        ),
        [
            pl.BlockSpec((orbital_count, GROUP, edge, LANES), lambda g, *s: (0, g, 0, 0)),
            pl.BlockSpec(edge_block, lambda g, *s: (0, jnp.maximum(g * GROUP - 1, 0), 0, 0)),
            pl.BlockSpec(
                edge_block, lambda g, *s: (0, jnp.minimum((g + 1) * GROUP, rows - 1), 0, 0)
            ),
            whole((orbital_count, edge, LANES)),
            whole((orbital_count, edge, LANES)),
        ]
        + [
            pl.BlockSpec((f.shape[0], GROUP, plane_count, LANES), lambda g, *s: (0, g, 0, 0))
            for f in fields
        ]
        + [group_spec((GROUP, edge, LANES), 0, start, count) for _, start, count, _ in firsts]
        + [
            group_spec((edge, lanes), 1, start, count)
            for pieces in (seconds, early)
            for _, start, count, _ in pieces
        ],
        [pl.BlockSpec((orbital_count, edge, lanes), lambda g, *s: (0, 0, g))],
        [jax.ShapeDtypeStruct(orbitals.shape, f32)],
        [
            pltpu.VMEM((2, edge + 2 * GROUP, LANES), f32),
            pltpu.VMEM((GROUP, REACH * plane_count, LANES), f32),
        ],
        groups,
        flops,
    )[0]

    return call(
        functools.partial(finish_kernel, slot_count - 1, [start for _, start, _, _ in late]),
        (asked, ids),
        (partial, *(piece for *_, piece in late)),
        [own_spec] + [group_spec((edge, lanes), 1, start, count) for _, start, count, _ in late],
        [own_spec],
        [jax.ShapeDtypeStruct(orbitals.shape, f32)],
        [],
        groups,
        flops,
    )[0]


def solution(mesh):
    placed = (P("slab", None, "sub"), P("slab", "sub"), P(), P("slab", None), P("slab"))
    return jax.shard_map(
        program, mesh=mesh, in_specs=placed, out_specs=P("slab", None, "sub"), check_vma=False
    )
```

```python
import functools
import math

import jax
import jax.numpy as jnp
import numpy as np
from jax import lax
from jax.experimental import pallas as pl
from jax.experimental.pallas import tpu as pltpu
from jax.sharding import PartitionSpec as P

REACH = 16
LANES = 128
GROUP = 8
VMEM_LIMIT = 20 << 20

SCREEN = 0.0008
FOCK_SHARE = 0.25
LOCAL_FACTOR = (3.0 / math.pi) ** (1.0 / 3.0)
EPSILON = 1e-06


def from_behind(value, axis, by):
    size = lax.axis_size(axis)
    return lax.ppermute(value, axis, [(i, (i + by) % size) for i in range(size)])


def partner(index, step, size):
    if size & (size - 1) == 0:
        return index ^ step
    return (size - index + step) % size


def exchange(pieces, axis):
    size = lax.axis_size(axis)
    received = []
    for step, piece in enumerate(pieces):
        pairs = [(i, partner(i, step, size)) for i in range(size)]
        if all(source == target for source, target in pairs):
            received.append(piece)
        else:
            received.append(lax.ppermute(piece, axis, pairs))
    return received


def split_bf16(value):
    high = value.astype(jnp.bfloat16)
    low = (value - high.astype(jnp.float32)).astype(jnp.bfloat16)
    return high, low


def sine_tables(box_edge):
    levels = np.arange(1, box_edge + 1, dtype=np.float64)
    sine = np.sqrt(2.0 / (box_edge + 1)) * np.sin(
        np.pi * levels[:, None] * levels[None, :] / (box_edge + 1)
    )
    sine = sine.astype(np.float32)
    high = sine.astype(jnp.bfloat16)
    low = (sine - high.astype(np.float32)).astype(jnp.bfloat16)
    padded = np.zeros((LANES, 2 * LANES), dtype=high.dtype)
    padded[:box_edge, :box_edge] = high
    padded[:box_edge, LANES : LANES + box_edge] = low
    stacked = np.concatenate([high, low], axis=0)
    return padded, stacked


def level_tables(box_edge):
    levels = np.arange(1, box_edge + 1, dtype=np.float64)
    levels = 2.0 - 2.0 * np.cos(np.pi * levels / (box_edge + 1))
    kept = box_edge * box_edge // LANES
    spare = LANES - box_edge
    low_rows = box_edge - kept
    columns = np.zeros((kept, LANES), np.float64)
    for row in range(kept):
        columns[row, :box_edge] = levels[row] + levels
        part = row // low_rows
        columns[row, box_edge:] = (
            levels[kept + row % low_rows] + levels[part * spare : (part + 1) * spare]
        )
    own = np.repeat(levels[:, None], 2 * LANES, axis=1)
    return columns.astype(np.float32), own.astype(np.float32)


def lane_index(shape):
    return lax.broadcasted_iota(jnp.int32, shape, len(shape) - 1)


def roll_lanes(value, shift):
    return pltpu.roll(value, shift, 1)


def unpack_quad(tiles, edge):
    first, second, third = tiles
    lane = lane_index(first.shape)
    spare = LANES - edge
    keep = lane < edge
    rows = [
        first,
        roll_lanes(jnp.where(lane >= edge, first, second), spare),
        roll_lanes(jnp.where(lane >= edge - spare, second, third), 2 * spare),
        roll_lanes(third, 3 * spare),
    ]
    return [jnp.where(keep, row, 0.0) for row in rows]


def pack_quad(rows, edge):
    zero, one, two, three = rows
    lane = lane_index(zero.shape)
    spare = LANES - edge
    one = roll_lanes(one, edge)
    two = roll_lanes(two, edge - spare)
    three = roll_lanes(three, spare)
    return [
        jnp.where(lane < edge, zero, one),
        jnp.where(lane < edge - spare, one, two),
        jnp.where(lane < spare, two, three),
    ]


def transform_lanes(value, padded_ref):
    high, low = split_bf16(value)
    both = jnp.dot(high, padded_ref[...], preferred_element_type=jnp.float32)
    rest = jnp.dot(low, padded_ref[:, :LANES], preferred_element_type=jnp.float32)
    return both[:, :LANES] + (both[:, LANES:] + rest)


def transform_rows(value, stacked_ref):
    edge = stacked_ref.shape[0] // 2
    high, low = split_bf16(value)
    both = jnp.dot(stacked_ref[...], high, preferred_element_type=jnp.float32)
    rest = jnp.dot(stacked_ref[:edge, :], low, preferred_element_type=jnp.float32)
    return both[:edge] + (both[edge:] + rest)


class Scalars:
    def __init__(self, refs, sizes):
        self.corners, self.pairs, self.count, self.ids = refs
        self.orbital_count, self.plane_count, self.grid_planes = sizes
        self.total = self.corners.shape[0]

    def position(self):
        return self.ids[0]

    def place(self):
        return self.ids[1]

    def window_start(self, orbital):
        first = self.corners[self.position() * self.orbital_count + orbital, 0]
        return lax.rem(
            first - self.position() * self.plane_count + self.grid_planes, self.grid_planes
        )

    def column(self, orbital):
        return self.corners[self.position() * self.orbital_count + orbital, 1]

    def member(self, slot, side):
        owned = self.pairs[slot, side] - self.position() * self.orbital_count
        return lax.rem(owned + self.total, self.total)

    def remote(self, slot):
        return self.member(slot, 1) >= self.orbital_count

    def kept(self, slot):
        return jnp.minimum(self.member(slot, 1), self.orbital_count - 1)

    def shifts(self, slot):
        first, second = self.pairs[slot, 0], self.pairs[slot, 1]
        half = self.grid_planes // 2
        along = self.corners[second, 0] - self.corners[first, 0] + half + self.grid_planes
        return (
            lax.rem(along, self.grid_planes) - half,
            self.corners[second, 1] - self.corners[first, 1],
        )

    def weight(self, slot):
        return jnp.where(slot < self.count[0], 1.0, 0.0).astype(jnp.float32)


def lane_shift(amount):
    return lax.rem(amount + LANES, LANES)


def spread_kernel(sizes, folds, corners, ids, dense_ref, *refs):
    scalars = Scalars((corners, None, None, ids), sizes)
    *window_refs, buffer = refs
    orbital_count, edge, _ = dense_ref.shape
    planes = window_refs[0].shape[2]
    window_planes = REACH * planes
    spread = window_planes - edge

    @pl.when(pl.program_id(0) == 0)
    def _():
        buffer[:, :, :spread, :] = jnp.zeros_like(buffer[:, :, :spread, :])
        buffer[:, :, spread + edge :, :] = jnp.zeros_like(buffer[:, :, spread + edge :, :])

    for orbital in range(orbital_count):
        for quad in range(GROUP // 4):
            tiles = [
                dense_ref[orbital, :, (3 * quad + t) * LANES : (3 * quad + t + 1) * LANES]
                for t in range(3)
            ]
            for r, row in enumerate(unpack_quad(tiles, edge)):
                buffer[orbital, 4 * quad + r, spread : spread + edge, :] = roll_lanes(
                    row * row, scalars.column(orbital)
                )
    for y in range(GROUP):
        total = None
        for orbital in range(orbital_count):
            start = spread - scalars.window_start(orbital)
            placed = buffer[orbital, y, pl.ds(start, window_planes), :]
            total = placed if total is None else total + placed
        for _ in range(folds):
            half = total.shape[0] // 2
            total = total[:half] + total[half:]
        for s in range(2 * len(window_refs)):
            window_refs[s // 2][s % 2, y] = total[s * planes : (s + 1) * planes]


def unpack_kernel(dense_ref, boxes_ref):
    orbital_count, edge, _ = dense_ref.shape
    for orbital in range(orbital_count):
        for quad in range(GROUP // 4):
            tiles = [
                dense_ref[orbital, :, (3 * quad + t) * LANES : (3 * quad + t + 1) * LANES]
                for t in range(3)
            ]
            for r, row in enumerate(unpack_quad(tiles, edge)):
                boxes_ref[orbital, 4 * quad + r] = row


def forward_kernel(sizes, sub_count, pad, slot, *refs):
    scalars = Scalars(refs[:4], sizes)
    own_ref, second_ref, dense_ref, padded_ref, stacked_ref = refs[4:9]
    outs = refs[9 : 9 + sub_count]
    moved_ref, buffer, flat = refs[9 + sub_count :]
    edge = own_ref.shape[2]
    remote = scalars.remote(slot)

    @pl.when(pl.program_id(0) == 0)
    def _():
        buffer[:, :pad, :] = jnp.zeros((GROUP, pad, LANES), jnp.float32)
        buffer[:, pad + edge :, :] = jnp.zeros((GROUP, pad, LANES), jnp.float32)

    @pl.when(remote)
    def _():
        for quad in range(GROUP // 4):
            tiles = [
                dense_ref[:, (3 * quad + t) * LANES : (3 * quad + t + 1) * LANES]
                for t in range(3)
            ]
            for r, row in enumerate(unpack_quad(tiles, edge)):
                buffer[4 * quad + r, pad : pad + edge, :] = row

    @pl.when(jnp.logical_not(remote))
    def _():
        buffer[:, pad : pad + edge, :] = second_ref[0]

    along, across = scalars.shifts(slot)
    lane = lane_index((edge, LANES))
    products = []
    for y in range(GROUP):
        moved = roll_lanes(buffer[y, pl.ds(pad - along, edge), :], lane_shift(across))
        moved = jnp.where(lane < edge, moved, 0.0)
        moved_ref[y] = moved
        products.append(own_ref[0, y] * moved)
    turned = transform_lanes(jnp.concatenate(products, axis=0), padded_ref)
    kept = edge * edge // LANES
    low_rows = edge - kept
    spare = LANES - edge
    keep = lane_index((kept, LANES)) < edge
    for y in range(0, GROUP, 2):
        pair = jnp.concatenate(
            [turned[(y + k) * edge : (y + k + 1) * edge] for k in range(2)], axis=1
        )
        pair = transform_rows(pair, stacked_ref)
        for k in range(2):
            spectral = pair[:, k * LANES : (k + 1) * LANES]
            low = spectral[kept:]
            tail = jnp.concatenate(
                [roll_lanes(low, edge - part * spare) for part in range(kept // low_rows)], axis=0
            )
            flat[pl.ds(y + k, kept, stride=GROUP), :] = jnp.where(keep, spectral[:kept], tail)
    chunk = kept // sub_count * GROUP
    for step in range(sub_count):
        target = partner(scalars.place(), step, sub_count)
        outs[step][0] = flat[pl.ds(pl.multiple_of(target * chunk, GROUP), chunk), :]


def solve_kernel(sizes, sub_count, inward, outward, *refs):
    scalars = Scalars(refs[:4], sizes)
    rest = refs[4:]
    pieces = rest[: len(inward) * sub_count]
    columns_ref, levels_ref, stacked_ref, *outs, work = rest[len(inward) * sub_count :]
    count = pieces[0].shape[1] // GROUP
    edge = stacked_ref.shape[0] // 2
    rows = edge // sub_count
    for part, (first_group, group_count) in enumerate(inward):
        for step in range(sub_count):
            source = partner(scalars.place(), step, sub_count)
            piece = pieces[part * sub_count + step]
            for g in range(group_count):
                base = pl.multiple_of(source * rows + (first_group + g) * GROUP, GROUP)
                for q in range(count):
                    work[q // 2, pl.ds(base, GROUP), (q % 2) * LANES : (q % 2 + 1) * LANES] = piece[
                        g, q * GROUP : (q + 1) * GROUP, :
                    ]
    first = scalars.place() * (count * pl.num_programs(0)) + pl.program_id(0) * count
    for pair in range(count // 2):
        spectral = transform_rows(work[pair], stacked_ref)
        column = jnp.concatenate(
            [columns_ref[pl.ds(first + 2 * pair + k, 1), :] for k in range(2)], axis=1
        )
        spectral = spectral * ((4.0 * math.pi) / (levels_ref[...] + column + SCREEN))
        work[pair] = transform_rows(spectral, stacked_ref)
    for step in range(sub_count):
        target = partner(scalars.place(), step, sub_count)
        for part, (first_group, group_count) in enumerate(outward):
            out = outs[part * sub_count + step]
            for g in range(group_count):
                base = pl.multiple_of(target * rows + (first_group + g) * GROUP, GROUP)
                for q in range(count):
                    out[g, q * GROUP : (q + 1) * GROUP, :] = work[
                        q // 2, pl.ds(base, GROUP), (q % 2) * LANES : (q % 2 + 1) * LANES
                    ]


def backward_kernel(sizes, sub_count, pad, slot, *refs):
    scalars = Scalars(refs[:4], sizes)
    rest = refs[4:]
    pieces = rest[:sub_count]
    own_ref, moved_ref, padded_ref, stacked_ref, first_ref, second_ref, buffer, flat = rest[
        sub_count:
    ]
    edge = own_ref.shape[2]
    weight = scalars.weight(slot)
    kept = edge * edge // LANES
    low_rows = edge - kept
    spare = LANES - edge
    chunk = kept // sub_count * GROUP

    @pl.when(pl.program_id(0) == 0)
    def _():
        buffer[:, :pad, :] = jnp.zeros((GROUP, pad, LANES), jnp.float32)
        buffer[:, pad + edge :, :] = jnp.zeros((GROUP, pad, LANES), jnp.float32)

    for step in range(sub_count):
        source = partner(scalars.place(), step, sub_count)
        flat[pl.ds(pl.multiple_of(source * chunk, GROUP), chunk), :] = pieces[step][0]
    lane = lane_index((low_rows, LANES))
    turned = []
    for y in range(0, GROUP, 2):
        pair = []
        for k in range(2):
            packed = flat[pl.ds(y + k, kept, stride=GROUP), :]
            low = None
            for part in range(kept // low_rows - 1, -1, -1):
                piece = roll_lanes(
                    packed[part * low_rows : (part + 1) * low_rows], (part + 1) * spare
                )
                low = piece if low is None else jnp.where(lane < (part + 1) * spare, piece, low)
            pair.append(jnp.concatenate([packed, low], axis=0))
        pair = transform_rows(jnp.concatenate(pair, axis=1), stacked_ref)
        turned += [pair[:, :LANES], pair[:, LANES:]]
    potential = transform_lanes(jnp.concatenate(turned, axis=0), padded_ref)
    along, across = scalars.shifts(slot)
    for quad in range(GROUP // 4):
        rows = []
        for r in range(4):
            y = 4 * quad + r
            solved = potential[y * edge : (y + 1) * edge] * weight
            first_ref[y] = solved * moved_ref[y]
            buffer[y, pad : pad + edge, :] = solved * own_ref[0, y]
            rows.append(roll_lanes(buffer[y, pl.ds(pad + along, edge), :], lane_shift(-across)))
        for t, tile in enumerate(pack_quad(rows, edge)):
            second_ref[:, (3 * quad + t) * LANES : (3 * quad + t + 1) * LANES] = tile


def at_group(pieces, refs, index):
    value = None
    for (_, start), ref in zip(pieces, refs):
        piece = ref[index]
        value = piece if value is None else jnp.where(pl.program_id(0) >= start, piece, value)
    return value


def combine_kernel(sizes, layout, *refs):
    scalars = Scalars(refs[:4], sizes)
    asked = refs[4]
    boxes_ref, before_ref, after_ref, low_ref, high_ref, *rest = refs[5:]
    out_ref, buffer = rest[-2:]
    by_slot = []
    for pieces in layout:
        slots = {}
        for piece, ref in zip(pieces, rest):
            slots.setdefault(piece[0], ([], []))
            slots[piece[0]][0].append(piece)
            slots[piece[0]][1].append(ref)
        by_slot.append(slots)
        rest = rest[len(pieces) :]
    firsts, seconds, early = by_slot
    orbital_count, _, edge, _ = boxes_ref.shape
    group = pl.program_id(0)
    last = pl.num_programs(0) - 1
    buffer[...] = jnp.zeros_like(buffer)

    def share(condition):
        return jnp.where(condition, FOCK_SHARE, 0.0)

    for orbital in range(orbital_count):
        owned = scalars.position() * orbital_count + orbital
        for quad in range(GROUP // 4):
            rows = []
            for r in range(4):
                y = 4 * quad + r
                box = boxes_ref[orbital, y]
                if y == 0:
                    behind = jnp.where(group == 0, low_ref[orbital], before_ref[orbital, 0])
                else:
                    behind = boxes_ref[orbital, y - 1]
                if y == GROUP - 1:
                    ahead = jnp.where(group == last, high_ref[orbital], after_ref[orbital, 0])
                else:
                    ahead = boxes_ref[orbital, y + 1]
                buffer[y % 2, GROUP : GROUP + edge, :] = box
                beside = buffer[y % 2, GROUP - 1 : GROUP - 1 + edge, :]
                beside = beside + buffer[y % 2, GROUP + 1 : GROUP + 1 + edge, :]
                beside = beside + (behind + ahead)
                beside = beside + (roll_lanes(box, 1) + roll_lanes(box, LANES - 1))
                value = 3.0 * box - 0.5 * beside
                for slot, (pieces, held) in firsts.items():
                    scale = share(scalars.member(slot, 0) == orbital)
                    value = value - scale * at_group(pieces, held, y)
                rows.append(value)
            for t, tile in enumerate(pack_quad(rows, edge)):
                lanes = slice((3 * quad + t) * LANES, (3 * quad + t + 1) * LANES)
                for slot, (pieces, held) in seconds.items():
                    scale = share(scalars.member(slot, 1) == orbital)
                    tile = tile - scale * at_group(pieces, held, (slice(None), lanes))
                for slot, (pieces, held) in early.items():
                    scale = share(asked[slot, 1] == owned)
                    tile = tile - scale * at_group(pieces, held, (slice(None), lanes))
                out_ref[orbital, :, lanes] = tile


def field_kernel(sizes, fields, folds, corners, ids, base_ref, boxes_ref, *rest):
    scalars = Scalars((corners, None, None, ids), sizes)
    out_ref, window = rest[-2:]
    field_refs = rest[:fields]
    orbital_count, _, edge, _ = boxes_ref.shape
    position = 0
    planes = field_refs[0].shape[2]
    half = (fields - 1) // 2
    sources = [field_refs[:1]] + [(field_refs[1 + k], field_refs[1 + half + k]) for k in range(half)]
    for pair in sources:
        for s in range(pair[0].shape[0]):
            for y in range(GROUP):
                value = pair[0][s, y]
                for ref in pair[1:]:
                    value = value + ref[s, y]
                for copy in range(2**folds):
                    start = (position + copy * (REACH // 2**folds)) * planes
                    window[y, start : start + planes, :] = value
            position += 1

    for orbital in range(orbital_count):
        begin = scalars.window_start(orbital)
        turn = lane_shift(-scalars.column(orbital))
        for quad in range(GROUP // 4):
            rows = []
            for r in range(4):
                y = 4 * quad + r
                field = roll_lanes(window[y, pl.ds(begin, edge), :], turn)
                rows.append(field * boxes_ref[orbital, y])
            for t, tile in enumerate(pack_quad(rows, edge)):
                lanes = slice((3 * quad + t) * LANES, (3 * quad + t + 1) * LANES)
                out_ref[orbital, :, lanes] = base_ref[orbital, :, lanes] + tile


def finish_kernel(slot, starts, asked, ids, partial_ref, *refs):
    out_ref = refs[-1]
    orbital_count = partial_ref.shape[0]
    value = at_group([(slot, start) for start in starts], refs[:-1], Ellipsis)
    for orbital in range(orbital_count):
        mine = asked[slot, 1] == ids[0] * orbital_count + orbital
        out_ref[orbital] = partial_ref[orbital] - jnp.where(mine, FOCK_SHARE, 0.0) * value


def whole(shape):
    return pl.BlockSpec(shape, lambda g, *s: (0,) * len(shape))


def call(kernel, scalars, operands, in_specs, out_specs, out_shape, scratch, groups, flops):
    return pl.pallas_call(
        kernel,
        grid_spec=pltpu.PrefetchScalarGridSpec(
            num_scalar_prefetch=len(scalars),
            grid=(groups,),
            in_specs=in_specs,
            out_specs=out_specs,
            scratch_shapes=scratch,
        ),
        out_shape=out_shape,
        cost_estimate=pl.CostEstimate(
            flops=flops, bytes_accessed=4_000_000, transcendentals=0
        ),
        compiler_params=pltpu.CompilerParams(
            dimension_semantics=("arbitrary",), vmem_limit_bytes=VMEM_LIMIT
        ),
    )(*scalars, *operands)


def program(orbitals, external_potential, corners, pair_list, pair_count):
    f32 = jnp.float32
    orbital_count, edge, merged = orbitals.shape
    rows = merged // edge
    groups = rows // GROUP
    lanes = GROUP * edge
    devices = lax.axis_size("slab")
    sub_count = lax.axis_size("sub")
    position = lax.axis_index("slab")
    place = lax.axis_index("sub")
    plane_count = external_potential.shape[0]
    grid_planes = plane_count * devices
    sizes = (orbital_count, plane_count, grid_planes)
    spread = REACH * plane_count - edge
    pad = spread + plane_count
    slot_count = pair_list.shape[0]
    kept = edge * edge // LANES
    chunk = kept // sub_count * GROUP
    folds = 0
    while (REACH >> (folds + 1)) >= 2 and (REACH >> (folds + 1)) % devices == 0:
        folds += 1
    slabs = REACH >> folds
    padded, stacked = (jnp.asarray(t) for t in sine_tables(edge))
    columns, own_levels = (jnp.asarray(t) for t in level_tables(edge))
    flops = 200_000_000
    ids = jnp.stack([position, place]).astype(jnp.int32)
    scalars = (corners, pair_list, pair_count, ids)

    asked = from_behind(pair_list, "slab", 1)

    box_shape = (orbital_count, rows, edge, LANES)
    own_spec = pl.BlockSpec((orbital_count, edge, lanes), lambda g, *s: (0, 0, g))
    windows = call(
        functools.partial(spread_kernel, sizes, folds),
        (corners, ids),
        (orbitals,),
        [own_spec],
        [pl.BlockSpec((2, GROUP, plane_count, LANES), lambda g, *s: (0, g, 0, 0))] * (slabs // 2),
        [jax.ShapeDtypeStruct((2, rows, plane_count, LANES), f32)] * (slabs // 2),
        [pltpu.VMEM((orbital_count, GROUP, edge + 2 * spread, LANES), f32)],
        groups,
        flops,
    )
    boxes = call(
        unpack_kernel,
        (),
        (orbitals,),
        [own_spec],
        [pl.BlockSpec((orbital_count, GROUP, edge, LANES), lambda g, *s: (0, g, 0, 0))],
        [jax.ShapeDtypeStruct(box_shape, f32)],
        [],
        groups,
        flops,
    )[0]

    near = windows[0]
    parts = []
    for hop in range(2, slabs, 2):
        parts.append(from_behind(windows[hop // 2], "slab", hop))
    for part in parts:
        near = near + part
    onward = from_behind(near[1], "slab", 1)
    density = (near[0] + onward).transpose(1, 0, 2).reshape(external_potential.shape)
    local_field = external_potential - LOCAL_FACTOR * jnp.cbrt(density + EPSILON)
    local_field = local_field.reshape(plane_count, rows, LANES).transpose(1, 0, 2)
    beyond = from_behind(local_field, "slab", -1)
    both = jnp.stack([local_field, beyond])
    fields = [both]
    for parity in (1, 0):
        for hop in range(2, slabs, 2):
            pairs = [(i, (i - hop) % devices) for i in range(parity, devices, 2)]
            fields.append(lax.ppermute(both, "slab", pairs))

    answers = []
    for k in range(slot_count):
        picked = lax.dynamic_index_in_dim(
            orbitals, lax.rem(asked[k, 1], orbital_count), 0, keepdims=False
        )
        answers.append(from_behind(picked, "slab", -1))

    forward = [(i, i + 1) for i in range(sub_count - 1)]
    backward = [(target, source) for source, target in forward]
    low_halo = lax.ppermute(boxes[:, rows - 1], "sub", forward)
    high_halo = lax.ppermute(boxes[:, 0], "sub", backward)

    def side(slot, pick, start=0):
        def index(g, c, p, n, d):
            scalar = Scalars((c, p, n, d), sizes)
            return (scalar.kept(slot) if pick else scalar.member(slot, 0), g + start, 0, 0)

        return pl.BlockSpec((1, GROUP, edge, LANES), index)

    row_spec = pl.BlockSpec((GROUP, edge, LANES), lambda g, *s: (g, 0, 0))
    dense_spec = pl.BlockSpec((edge, lanes), lambda g, *s: (0, g))
    piece_spec = pl.BlockSpec((1, chunk, LANES), lambda g, *s: (g, 0, 0))
    shifted = pltpu.VMEM((GROUP, edge + 2 * pad, LANES), f32)
    flat = pltpu.VMEM((kept * GROUP, LANES), f32)
    solve_steps = 3
    tall = chunk // solve_steps
    tall_spec = pl.BlockSpec((groups, tall, LANES), lambda g, *s: (0, g, 0))
    firsts, seconds, returns = [], [], []
    pieced = [(0, 1), (1, groups - 1)] if groups > 1 else [(0, groups)]

    def tall_specs(parts):
        return [
            pl.BlockSpec((count, tall, LANES), lambda g, *s: (0, g, 0))
            for _, count in parts
            for _ in range(sub_count)
        ]

    def rows_from(start):
        return pl.BlockSpec((GROUP, edge, LANES), lambda g, *s: (g + start, 0, 0))

    for slot in range(slot_count):
        inward = [(0, groups)]
        pieces = []
        moved = {}
        for start, count in inward:
            outs = call(
                functools.partial(forward_kernel, sizes, sub_count, pad, slot),
                scalars,
                (boxes, boxes, answers[slot], padded, stacked),
                [
                    side(slot, 0, start),
                    side(slot, 1, start),
                    pl.BlockSpec((edge, lanes), lambda g, *s, start=start: (0, g + start)),
                    whole(padded.shape),
                    whole(stacked.shape),
                ],
                [piece_spec] * sub_count + [row_spec],
                [jax.ShapeDtypeStruct((count, chunk, LANES), f32)] * sub_count
                + [jax.ShapeDtypeStruct((count * GROUP, edge, LANES), f32)],
                [shifted, flat],
                count,
                flops * count // groups,
            )
            moved[start] = outs[sub_count]
            pieces += exchange(outs[:sub_count], "sub")
        outward = pieced
        solved = call(
            functools.partial(solve_kernel, sizes, sub_count, inward, outward),
            scalars,
            (*pieces, columns, own_levels, stacked),
            tall_specs(inward)
            + [whole(columns.shape), whole(own_levels.shape), whole(stacked.shape)],
            tall_specs(outward),
            [
                jax.ShapeDtypeStruct((count, chunk, LANES), f32)
                for _, count in outward
                for _ in range(sub_count)
            ],
            [pltpu.VMEM((tall // GROUP // 2, edge, 2 * LANES), f32)],
            solve_steps,
            flops,
        )
        received = [
            exchange(solved[part * sub_count : (part + 1) * sub_count], "sub")
            for part in range(len(outward))
        ]
        for part, (start, count) in enumerate(outward):
            origin = max(first for first in moved if first <= start)
            first, second = call(
                functools.partial(backward_kernel, sizes, sub_count, pad, slot),
                scalars,
                (*received[part], boxes, moved[origin], padded, stacked),
                [piece_spec] * sub_count
                + [
                    side(slot, 0, start),
                    rows_from(start - origin),
                    whole(padded.shape),
                    whole(stacked.shape),
                ],
                [row_spec, dense_spec],
                [
                    jax.ShapeDtypeStruct((count * GROUP, edge, LANES), f32),
                    jax.ShapeDtypeStruct((edge, count * lanes), f32),
                ],
                [shifted, flat],
                count,
                flops * count // groups,
            )
            firsts.append((slot, start, count, first))
            seconds.append((slot, start, count, second))
            returns.append((slot, start, count, from_behind(second, "slab", 1)))

    def group_spec(shape, axis, start, count):
        def index(g, *s):
            at = [0] * len(shape)
            at[axis] = jnp.clip(g - start, 0, count - 1)
            return tuple(at)

        return pl.BlockSpec(shape, index)

    early = [r for r in returns if r[0] < slot_count - 1]
    late = [r for r in returns if r[0] == slot_count - 1]
    layout = [
        [(slot, start) for slot, start, _, _ in pieces] for pieces in (firsts, seconds, early)
    ]
    edge_block = (orbital_count, 1, edge, LANES)
    partial = call(
        functools.partial(combine_kernel, sizes, layout),
        (*scalars, asked),
        (
            boxes,
            boxes,
            boxes,
            low_halo,
            high_halo,
            *(piece for pieces in (firsts, seconds, early) for *_, piece in pieces),
        ),
        [
            pl.BlockSpec((orbital_count, GROUP, edge, LANES), lambda g, *s: (0, g, 0, 0)),
            pl.BlockSpec(edge_block, lambda g, *s: (0, jnp.maximum(g * GROUP - 1, 0), 0, 0)),
            pl.BlockSpec(
                edge_block, lambda g, *s: (0, jnp.minimum((g + 1) * GROUP, rows - 1), 0, 0)
            ),
            whole((orbital_count, edge, LANES)),
            whole((orbital_count, edge, LANES)),
        ]
        + [group_spec((GROUP, edge, LANES), 0, start, count) for _, start, count, _ in firsts]
        + [
            group_spec((edge, lanes), 1, start, count)
            for pieces in (seconds, early)
            for _, start, count, _ in pieces
        ],
        [pl.BlockSpec((orbital_count, edge, lanes), lambda g, *s: (0, 0, g))],
        [jax.ShapeDtypeStruct(orbitals.shape, f32)],
        [pltpu.VMEM((2, edge + 2 * GROUP, LANES), f32)],
        groups,
        flops,
    )[0]
    partial = call(
        functools.partial(field_kernel, sizes, len(fields), folds),
        (corners, ids),
        (partial, boxes, *fields),
        [own_spec, pl.BlockSpec((orbital_count, GROUP, edge, LANES), lambda g, *s: (0, g, 0, 0))]
        + [
            pl.BlockSpec((f.shape[0], GROUP, plane_count, LANES), lambda g, *s: (0, g, 0, 0))
            for f in fields
        ],
        [own_spec],
        [jax.ShapeDtypeStruct(orbitals.shape, f32)],
        [pltpu.VMEM((GROUP, REACH * plane_count, LANES), f32)],
        groups,
        flops,
    )[0]

    return call(
        functools.partial(finish_kernel, slot_count - 1, [start for _, start, _, _ in late]),
        (asked, ids),
        (partial, *(piece for *_, piece in late)),
        [own_spec] + [group_spec((edge, lanes), 1, start, count) for _, start, count, _ in late],
        [own_spec],
        [jax.ShapeDtypeStruct(orbitals.shape, f32)],
        [],
        groups,
        flops,
    )[0]


def solution(mesh):
    placed = (P("slab", None, "sub"), P("slab", "sub"), P(), P("slab", None), P("slab"))
    return jax.shard_map(
        program, mesh=mesh, in_specs=placed, out_specs=P("slab", None, "sub"), check_vma=False
    )
```

```python
import functools
import math

import jax
import jax.numpy as jnp
import numpy as np
from jax import lax
from jax.experimental import pallas as pl
from jax.experimental.pallas import tpu as pltpu
from jax.sharding import PartitionSpec as P

REACH = 16
LANES = 128
GROUP = 8
VMEM_LIMIT = 20 << 20

SCREEN = 0.0008
FOCK_SHARE = 0.25
LOCAL_FACTOR = (3.0 / math.pi) ** (1.0 / 3.0)
EPSILON = 1e-06


def from_behind(value, axis, by):
    size = lax.axis_size(axis)
    return lax.ppermute(value, axis, [(i, (i + by) % size) for i in range(size)])


def partner(index, step, size):
    if size & (size - 1) == 0:
        return index ^ step
    return (size - index + step) % size


def exchange(pieces, axis):
    size = lax.axis_size(axis)
    received = []
    for step, piece in enumerate(pieces):
        pairs = [(i, partner(i, step, size)) for i in range(size)]
        if all(source == target for source, target in pairs):
            received.append(piece)
        else:
            received.append(lax.ppermute(piece, axis, pairs))
    return received


def split_bf16(value):
    high = value.astype(jnp.bfloat16)
    low = (value - high.astype(jnp.float32)).astype(jnp.bfloat16)
    return high, low


def sine_tables(box_edge):
    levels = np.arange(1, box_edge + 1, dtype=np.float64)
    sine = np.sqrt(2.0 / (box_edge + 1)) * np.sin(
        np.pi * levels[:, None] * levels[None, :] / (box_edge + 1)
    )
    sine = sine.astype(np.float32)
    high = sine.astype(jnp.bfloat16)
    low = (sine - high.astype(np.float32)).astype(jnp.bfloat16)
    padded = np.zeros((LANES, 2 * LANES), dtype=high.dtype)
    padded[:box_edge, :box_edge] = high
    padded[:box_edge, LANES : LANES + box_edge] = low
    stacked = np.concatenate([high, low], axis=0)
    return padded, stacked


def level_tables(box_edge):
    levels = np.arange(1, box_edge + 1, dtype=np.float64)
    levels = 2.0 - 2.0 * np.cos(np.pi * levels / (box_edge + 1))
    kept = box_edge * box_edge // LANES
    spare = LANES - box_edge
    low_rows = box_edge - kept
    columns = np.zeros((kept, LANES), np.float64)
    for row in range(kept):
        columns[row, :box_edge] = levels[row] + levels
        part = row // low_rows
        columns[row, box_edge:] = (
            levels[kept + row % low_rows] + levels[part * spare : (part + 1) * spare]
        )
    own = np.repeat(levels[:, None], 2 * LANES, axis=1)
    return columns.astype(np.float32), own.astype(np.float32)


def lane_index(shape):
    return lax.broadcasted_iota(jnp.int32, shape, len(shape) - 1)


def roll_lanes(value, shift):
    return pltpu.roll(value, shift, 1)


def unpack_quad(tiles, edge):
    first, second, third = tiles
    lane = lane_index(first.shape)
    spare = LANES - edge
    keep = lane < edge
    rows = [
        first,
        roll_lanes(jnp.where(lane >= edge, first, second), spare),
        roll_lanes(jnp.where(lane >= edge - spare, second, third), 2 * spare),
        roll_lanes(third, 3 * spare),
    ]
    return [jnp.where(keep, row, 0.0) for row in rows]


def pack_quad(rows, edge):
    zero, one, two, three = rows
    lane = lane_index(zero.shape)
    spare = LANES - edge
    one = roll_lanes(one, edge)
    two = roll_lanes(two, edge - spare)
    three = roll_lanes(three, spare)
    return [
        jnp.where(lane < edge, zero, one),
        jnp.where(lane < edge - spare, one, two),
        jnp.where(lane < spare, two, three),
    ]


def transform_lanes(value, padded_ref):
    high, low = split_bf16(value)
    both = jnp.dot(high, padded_ref[...], preferred_element_type=jnp.float32)
    rest = jnp.dot(low, padded_ref[:, :LANES], preferred_element_type=jnp.float32)
    return both[:, :LANES] + (both[:, LANES:] + rest)


def transform_rows(value, stacked_ref):
    edge = stacked_ref.shape[0] // 2
    high, low = split_bf16(value)
    both = jnp.dot(stacked_ref[...], high, preferred_element_type=jnp.float32)
    rest = jnp.dot(stacked_ref[:edge, :], low, preferred_element_type=jnp.float32)
    return both[:edge] + (both[edge:] + rest)


class Scalars:
    def __init__(self, refs, sizes):
        self.corners, self.pairs, self.count, self.ids = refs
        self.orbital_count, self.plane_count, self.grid_planes = sizes
        self.total = self.corners.shape[0]

    def position(self):
        return self.ids[0]

    def place(self):
        return self.ids[1]

    def window_start(self, orbital):
        first = self.corners[self.position() * self.orbital_count + orbital, 0]
        return lax.rem(
            first - self.position() * self.plane_count + self.grid_planes, self.grid_planes
        )

    def column(self, orbital):
        return self.corners[self.position() * self.orbital_count + orbital, 1]

    def member(self, slot, side):
        owned = self.pairs[slot, side] - self.position() * self.orbital_count
        return lax.rem(owned + self.total, self.total)

    def remote(self, slot):
        return self.member(slot, 1) >= self.orbital_count

    def kept(self, slot):
        return jnp.minimum(self.member(slot, 1), self.orbital_count - 1)

    def shifts(self, slot):
        first, second = self.pairs[slot, 0], self.pairs[slot, 1]
        half = self.grid_planes // 2
        along = self.corners[second, 0] - self.corners[first, 0] + half + self.grid_planes
        return (
            lax.rem(along, self.grid_planes) - half,
            self.corners[second, 1] - self.corners[first, 1],
        )

    def weight(self, slot):
        return jnp.where(slot < self.count[0], 1.0, 0.0).astype(jnp.float32)


def lane_shift(amount):
    return lax.rem(amount + LANES, LANES)


def spread_kernel(sizes, folds, corners, ids, dense_ref, *refs):
    scalars = Scalars((corners, None, None, ids), sizes)
    *window_refs, buffer = refs
    orbital_count, edge, _ = dense_ref.shape
    planes = window_refs[0].shape[2]
    window_planes = REACH * planes
    spread = window_planes - edge

    @pl.when(pl.program_id(0) == 0)
    def _():
        buffer[:, :, :spread, :] = jnp.zeros_like(buffer[:, :, :spread, :])
        buffer[:, :, spread + edge :, :] = jnp.zeros_like(buffer[:, :, spread + edge :, :])

    for orbital in range(orbital_count):
        for quad in range(GROUP // 4):
            tiles = [
                dense_ref[orbital, :, (3 * quad + t) * LANES : (3 * quad + t + 1) * LANES]
                for t in range(3)
            ]
            for r, row in enumerate(unpack_quad(tiles, edge)):
                buffer[orbital, 4 * quad + r, spread : spread + edge, :] = roll_lanes(
                    row * row, scalars.column(orbital)
                )
    for y in range(GROUP):
        total = None
        for orbital in range(orbital_count):
            start = spread - scalars.window_start(orbital)
            placed = buffer[orbital, y, pl.ds(start, window_planes), :]
            total = placed if total is None else total + placed
        for _ in range(folds):
            half = total.shape[0] // 2
            total = total[:half] + total[half:]
        for s in range(2 * len(window_refs)):
            window_refs[s // 2][s % 2, y] = total[s * planes : (s + 1) * planes]


def unpack_kernel(dense_ref, boxes_ref):
    orbital_count, edge, _ = dense_ref.shape
    for orbital in range(orbital_count):
        for quad in range(GROUP // 4):
            tiles = [
                dense_ref[orbital, :, (3 * quad + t) * LANES : (3 * quad + t + 1) * LANES]
                for t in range(3)
            ]
            for r, row in enumerate(unpack_quad(tiles, edge)):
                boxes_ref[orbital, 4 * quad + r] = row


def forward_kernel(sizes, sub_count, pad, slot, *refs):
    scalars = Scalars(refs[:4], sizes)
    own_ref, second_ref, dense_ref, padded_ref, stacked_ref = refs[4:9]
    outs = refs[9 : 9 + sub_count]
    moved_ref, buffer, flat = refs[9 + sub_count :]
    edge = own_ref.shape[2]
    remote = scalars.remote(slot)

    @pl.when(pl.program_id(0) == 0)
    def _():
        buffer[:, :pad, :] = jnp.zeros((GROUP, pad, LANES), jnp.float32)
        buffer[:, pad + edge :, :] = jnp.zeros((GROUP, pad, LANES), jnp.float32)

    @pl.when(remote)
    def _():
        for quad in range(GROUP // 4):
            tiles = [
                dense_ref[:, (3 * quad + t) * LANES : (3 * quad + t + 1) * LANES]
                for t in range(3)
            ]
            for r, row in enumerate(unpack_quad(tiles, edge)):
                buffer[4 * quad + r, pad : pad + edge, :] = row

    @pl.when(jnp.logical_not(remote))
    def _():
        buffer[:, pad : pad + edge, :] = second_ref[0]

    along, across = scalars.shifts(slot)
    lane = lane_index((edge, LANES))
    products = []
    for y in range(GROUP):
        moved = roll_lanes(buffer[y, pl.ds(pad - along, edge), :], lane_shift(across))
        moved = jnp.where(lane < edge, moved, 0.0)
        moved_ref[y] = moved
        products.append(own_ref[0, y] * moved)
    turned = transform_lanes(jnp.concatenate(products, axis=0), padded_ref)
    kept = edge * edge // LANES
    low_rows = edge - kept
    spare = LANES - edge
    keep = lane_index((kept, LANES)) < edge
    for y in range(0, GROUP, 2):
        pair = jnp.concatenate(
            [turned[(y + k) * edge : (y + k + 1) * edge] for k in range(2)], axis=1
        )
        pair = transform_rows(pair, stacked_ref)
        for k in range(2):
            spectral = pair[:, k * LANES : (k + 1) * LANES]
            low = spectral[kept:]
            tail = jnp.concatenate(
                [roll_lanes(low, edge - part * spare) for part in range(kept // low_rows)], axis=0
            )
            flat[pl.ds(y + k, kept, stride=GROUP), :] = jnp.where(keep, spectral[:kept], tail)
    chunk = kept // sub_count * GROUP
    for step in range(sub_count):
        target = partner(scalars.place(), step, sub_count)
        outs[step][0] = flat[pl.ds(pl.multiple_of(target * chunk, GROUP), chunk), :]


def solve_kernel(sizes, sub_count, inward, outward, *refs):
    scalars = Scalars(refs[:4], sizes)
    rest = refs[4:]
    pieces = rest[: len(inward) * sub_count]
    columns_ref, levels_ref, stacked_ref, *outs, work = rest[len(inward) * sub_count :]
    count = pieces[0].shape[1] // GROUP
    edge = stacked_ref.shape[0] // 2
    rows = edge // sub_count
    for part, (first_group, group_count) in enumerate(inward):
        for step in range(sub_count):
            source = partner(scalars.place(), step, sub_count)
            piece = pieces[part * sub_count + step]
            for g in range(group_count):
                base = pl.multiple_of(source * rows + (first_group + g) * GROUP, GROUP)
                for q in range(count):
                    work[q // 2, pl.ds(base, GROUP), (q % 2) * LANES : (q % 2 + 1) * LANES] = piece[
                        g, q * GROUP : (q + 1) * GROUP, :
                    ]
    first = scalars.place() * (count * pl.num_programs(0)) + pl.program_id(0) * count
    for pair in range(count // 2):
        spectral = transform_rows(work[pair], stacked_ref)
        column = jnp.concatenate(
            [columns_ref[pl.ds(first + 2 * pair + k, 1), :] for k in range(2)], axis=1
        )
        spectral = spectral * ((4.0 * math.pi) / (levels_ref[...] + column + SCREEN))
        work[pair] = transform_rows(spectral, stacked_ref)
    for step in range(sub_count):
        target = partner(scalars.place(), step, sub_count)
        for part, (first_group, group_count) in enumerate(outward):
            out = outs[part * sub_count + step]
            for g in range(group_count):
                base = pl.multiple_of(target * rows + (first_group + g) * GROUP, GROUP)
                for q in range(count):
                    out[g, q * GROUP : (q + 1) * GROUP, :] = work[
                        q // 2, pl.ds(base, GROUP), (q % 2) * LANES : (q % 2 + 1) * LANES
                    ]


def backward_kernel(sizes, sub_count, pad, slot, *refs):
    scalars = Scalars(refs[:4], sizes)
    rest = refs[4:]
    pieces = rest[:sub_count]
    own_ref, moved_ref, padded_ref, stacked_ref, first_ref, second_ref, buffer, flat = rest[
        sub_count:
    ]
    edge = own_ref.shape[2]
    weight = scalars.weight(slot)
    kept = edge * edge // LANES
    low_rows = edge - kept
    spare = LANES - edge
    chunk = kept // sub_count * GROUP

    @pl.when(pl.program_id(0) == 0)
    def _():
        buffer[:, :pad, :] = jnp.zeros((GROUP, pad, LANES), jnp.float32)
        buffer[:, pad + edge :, :] = jnp.zeros((GROUP, pad, LANES), jnp.float32)

    for step in range(sub_count):
        source = partner(scalars.place(), step, sub_count)
        flat[pl.ds(pl.multiple_of(source * chunk, GROUP), chunk), :] = pieces[step][0]
    lane = lane_index((low_rows, LANES))
    turned = []
    for y in range(0, GROUP, 2):
        pair = []
        for k in range(2):
            packed = flat[pl.ds(y + k, kept, stride=GROUP), :]
            low = None
            for part in range(kept // low_rows - 1, -1, -1):
                piece = roll_lanes(
                    packed[part * low_rows : (part + 1) * low_rows], (part + 1) * spare
                )
                low = piece if low is None else jnp.where(lane < (part + 1) * spare, piece, low)
            pair.append(jnp.concatenate([packed, low], axis=0))
        pair = transform_rows(jnp.concatenate(pair, axis=1), stacked_ref)
        turned += [pair[:, :LANES], pair[:, LANES:]]
    potential = transform_lanes(jnp.concatenate(turned, axis=0), padded_ref)
    along, across = scalars.shifts(slot)
    for quad in range(GROUP // 4):
        rows = []
        for r in range(4):
            y = 4 * quad + r
            solved = potential[y * edge : (y + 1) * edge] * weight
            first_ref[y] = solved * moved_ref[y]
            buffer[y, pad : pad + edge, :] = solved * own_ref[0, y]
            rows.append(roll_lanes(buffer[y, pl.ds(pad + along, edge), :], lane_shift(-across)))
        for t, tile in enumerate(pack_quad(rows, edge)):
            second_ref[:, (3 * quad + t) * LANES : (3 * quad + t + 1) * LANES] = tile


def at_group(pieces, refs, index):
    value = None
    for (_, start), ref in zip(pieces, refs):
        piece = ref[index]
        value = piece if value is None else jnp.where(pl.program_id(0) >= start, piece, value)
    return value


def combine_kernel(sizes, layout, *refs):
    scalars = Scalars(refs[:4], sizes)
    asked = refs[4]
    boxes_ref, before_ref, after_ref, low_ref, high_ref, *rest = refs[5:]
    out_ref, buffer = rest[-2:]
    by_slot = []
    for pieces in layout:
        slots = {}
        for piece, ref in zip(pieces, rest):
            slots.setdefault(piece[0], ([], []))
            slots[piece[0]][0].append(piece)
            slots[piece[0]][1].append(ref)
        by_slot.append(slots)
        rest = rest[len(pieces) :]
    firsts, seconds, early = by_slot
    orbital_count, _, edge, _ = boxes_ref.shape
    group = pl.program_id(0)
    last = pl.num_programs(0) - 1
    buffer[...] = jnp.zeros_like(buffer)

    def share(condition):
        return jnp.where(condition, FOCK_SHARE, 0.0)

    for orbital in range(orbital_count):
        owned = scalars.position() * orbital_count + orbital
        for quad in range(GROUP // 4):
            rows = []
            for r in range(4):
                y = 4 * quad + r
                box = boxes_ref[orbital, y]
                if y == 0:
                    behind = jnp.where(group == 0, low_ref[orbital], before_ref[orbital, 0])
                else:
                    behind = boxes_ref[orbital, y - 1]
                if y == GROUP - 1:
                    ahead = jnp.where(group == last, high_ref[orbital], after_ref[orbital, 0])
                else:
                    ahead = boxes_ref[orbital, y + 1]
                buffer[y % 2, GROUP : GROUP + edge, :] = box
                beside = buffer[y % 2, GROUP - 1 : GROUP - 1 + edge, :]
                beside = beside + buffer[y % 2, GROUP + 1 : GROUP + 1 + edge, :]
                beside = beside + (behind + ahead)
                beside = beside + (roll_lanes(box, 1) + roll_lanes(box, LANES - 1))
                value = 3.0 * box - 0.5 * beside
                for slot, (pieces, held) in firsts.items():
                    scale = share(scalars.member(slot, 0) == orbital)
                    value = value - scale * at_group(pieces, held, y)
                rows.append(value)
            for t, tile in enumerate(pack_quad(rows, edge)):
                lanes = slice((3 * quad + t) * LANES, (3 * quad + t + 1) * LANES)
                for slot, (pieces, held) in seconds.items():
                    scale = share(scalars.member(slot, 1) == orbital)
                    tile = tile - scale * at_group(pieces, held, (slice(None), lanes))
                for slot, (pieces, held) in early.items():
                    scale = share(asked[slot, 1] == owned)
                    tile = tile - scale * at_group(pieces, held, (slice(None), lanes))
                out_ref[orbital, :, lanes] = tile


def field_kernel(sizes, fields, folds, corners, ids, base_ref, boxes_ref, *rest):
    scalars = Scalars((corners, None, None, ids), sizes)
    out_ref, window = rest[-2:]
    field_refs = rest[:fields]
    orbital_count, _, edge, _ = boxes_ref.shape
    position = 0
    planes = field_refs[0].shape[2]
    half = (fields - 1) // 2
    sources = [field_refs[:1]] + [(field_refs[1 + k], field_refs[1 + half + k]) for k in range(half)]
    for pair in sources:
        for s in range(pair[0].shape[0]):
            for y in range(GROUP):
                value = pair[0][s, y]
                for ref in pair[1:]:
                    value = value + ref[s, y]
                for copy in range(2**folds):
                    start = (position + copy * (REACH // 2**folds)) * planes
                    window[y, start : start + planes, :] = value
            position += 1

    for orbital in range(orbital_count):
        begin = scalars.window_start(orbital)
        turn = lane_shift(-scalars.column(orbital))
        for quad in range(GROUP // 4):
            rows = []
            for r in range(4):
                y = 4 * quad + r
                field = roll_lanes(window[y, pl.ds(begin, edge), :], turn)
                rows.append(field * boxes_ref[orbital, y])
            for t, tile in enumerate(pack_quad(rows, edge)):
                lanes = slice((3 * quad + t) * LANES, (3 * quad + t + 1) * LANES)
                out_ref[orbital, :, lanes] = base_ref[orbital, :, lanes] + tile


def settle_kernel(slot, starts, bound, asked, ids, partial_ref, *refs):
    out_ref = refs[-1]
    orbital_count = partial_ref.shape[0]
    value = at_group([(slot, start) for start in starts], refs[:-1], Ellipsis)
    for orbital in range(orbital_count):
        mine = asked[slot, 1] == ids[0] * orbital_count + orbital
        mine = jnp.logical_and(mine, pl.program_id(0) < bound)
        out_ref[orbital] = partial_ref[orbital] - jnp.where(mine, FOCK_SHARE, 0.0) * value


def finish_kernel(orbital_count, slot, asked, ids, settled_ref, partial_ref, late_ref, out_ref):
    owned = asked[slot, 1] - ids[0] * orbital_count
    mine = jnp.logical_and(owned >= 0, owned < orbital_count)
    out_ref[0] = partial_ref[0] - jnp.where(mine, FOCK_SHARE, 0.0) * late_ref[...]


def whole(shape):
    return pl.BlockSpec(shape, lambda g, *s: (0,) * len(shape))


def call(
    kernel, scalars, operands, in_specs, out_specs, out_shape, scratch, groups, flops, aliases={}
):
    return pl.pallas_call(
        kernel,
        grid_spec=pltpu.PrefetchScalarGridSpec(
            num_scalar_prefetch=len(scalars),
            grid=(groups,),
            in_specs=in_specs,
            out_specs=out_specs,
            scratch_shapes=scratch,
        ),
        out_shape=out_shape,
        input_output_aliases=aliases,
        cost_estimate=pl.CostEstimate(
            flops=flops, bytes_accessed=4_000_000, transcendentals=0
        ),
        compiler_params=pltpu.CompilerParams(
            dimension_semantics=("arbitrary",), vmem_limit_bytes=VMEM_LIMIT
        ),
    )(*scalars, *operands)


def program(orbitals, external_potential, corners, pair_list, pair_count):
    f32 = jnp.float32
    orbital_count, edge, merged = orbitals.shape
    rows = merged // edge
    groups = rows // GROUP
    lanes = GROUP * edge
    devices = lax.axis_size("slab")
    sub_count = lax.axis_size("sub")
    position = lax.axis_index("slab")
    place = lax.axis_index("sub")
    plane_count = external_potential.shape[0]
    grid_planes = plane_count * devices
    sizes = (orbital_count, plane_count, grid_planes)
    spread = REACH * plane_count - edge
    pad = spread + plane_count
    slot_count = pair_list.shape[0]
    kept = edge * edge // LANES
    chunk = kept // sub_count * GROUP
    folds = 0
    while (REACH >> (folds + 1)) >= 2 and (REACH >> (folds + 1)) % devices == 0:
        folds += 1
    slabs = REACH >> folds
    padded, stacked = (jnp.asarray(t) for t in sine_tables(edge))
    columns, own_levels = (jnp.asarray(t) for t in level_tables(edge))
    flops = 200_000_000
    ids = jnp.stack([position, place]).astype(jnp.int32)
    scalars = (corners, pair_list, pair_count, ids)

    asked = from_behind(pair_list, "slab", 1)

    box_shape = (orbital_count, rows, edge, LANES)
    own_spec = pl.BlockSpec((orbital_count, edge, lanes), lambda g, *s: (0, 0, g))
    windows = call(
        functools.partial(spread_kernel, sizes, folds),
        (corners, ids),
        (orbitals,),
        [own_spec],
        [pl.BlockSpec((2, GROUP, plane_count, LANES), lambda g, *s: (0, g, 0, 0))] * (slabs // 2),
        [jax.ShapeDtypeStruct((2, rows, plane_count, LANES), f32)] * (slabs // 2),
        [pltpu.VMEM((orbital_count, GROUP, edge + 2 * spread, LANES), f32)],
        groups,
        flops,
    )
    boxes = call(
        unpack_kernel,
        (),
        (orbitals,),
        [own_spec],
        [pl.BlockSpec((orbital_count, GROUP, edge, LANES), lambda g, *s: (0, g, 0, 0))],
        [jax.ShapeDtypeStruct(box_shape, f32)],
        [],
        groups,
        flops,
    )[0]

    near = windows[0]
    parts = []
    for hop in range(2, slabs, 2):
        parts.append(from_behind(windows[hop // 2], "slab", hop))
    for part in parts:
        near = near + part
    onward = from_behind(near[1], "slab", 1)
    density = (near[0] + onward).transpose(1, 0, 2).reshape(external_potential.shape)
    local_field = external_potential - LOCAL_FACTOR * jnp.cbrt(density + EPSILON)
    local_field = local_field.reshape(plane_count, rows, LANES).transpose(1, 0, 2)
    beyond = from_behind(local_field, "slab", -1)
    both = jnp.stack([local_field, beyond])
    fields = [both]
    for parity in (1, 0):
        for hop in range(2, slabs, 2):
            pairs = [(i, (i - hop) % devices) for i in range(parity, devices, 2)]
            fields.append(lax.ppermute(both, "slab", pairs))

    answers = []
    for k in range(slot_count):
        picked = lax.dynamic_index_in_dim(
            orbitals, lax.rem(asked[k, 1], orbital_count), 0, keepdims=False
        )
        answers.append(from_behind(picked, "slab", -1))

    forward = [(i, i + 1) for i in range(sub_count - 1)]
    backward = [(target, source) for source, target in forward]
    low_halo = lax.ppermute(boxes[:, rows - 1], "sub", forward)
    high_halo = lax.ppermute(boxes[:, 0], "sub", backward)

    def side(slot, pick, start=0):
        def index(g, c, p, n, d):
            scalar = Scalars((c, p, n, d), sizes)
            return (scalar.kept(slot) if pick else scalar.member(slot, 0), g + start, 0, 0)

        return pl.BlockSpec((1, GROUP, edge, LANES), index)

    row_spec = pl.BlockSpec((GROUP, edge, LANES), lambda g, *s: (g, 0, 0))
    dense_spec = pl.BlockSpec((edge, lanes), lambda g, *s: (0, g))
    piece_spec = pl.BlockSpec((1, chunk, LANES), lambda g, *s: (g, 0, 0))
    shifted = pltpu.VMEM((GROUP, edge + 2 * pad, LANES), f32)
    flat = pltpu.VMEM((kept * GROUP, LANES), f32)
    solve_steps = 3
    tall = chunk // solve_steps
    tall_spec = pl.BlockSpec((groups, tall, LANES), lambda g, *s: (0, g, 0))
    firsts, seconds, returns = [], [], []
    pieced = [(0, 1), (1, groups - 1)] if groups > 1 else [(0, groups)]

    def tall_specs(parts):
        return [
            pl.BlockSpec((count, tall, LANES), lambda g, *s: (0, g, 0))
            for _, count in parts
            for _ in range(sub_count)
        ]

    def rows_from(start):
        return pl.BlockSpec((GROUP, edge, LANES), lambda g, *s: (g + start, 0, 0))

    for slot in range(slot_count):
        inward = [(0, groups)]
        pieces = []
        moved = {}
        for start, count in inward:
            outs = call(
                functools.partial(forward_kernel, sizes, sub_count, pad, slot),
                scalars,
                (boxes, boxes, answers[slot], padded, stacked),
                [
                    side(slot, 0, start),
                    side(slot, 1, start),
                    pl.BlockSpec((edge, lanes), lambda g, *s, start=start: (0, g + start)),
                    whole(padded.shape),
                    whole(stacked.shape),
                ],
                [piece_spec] * sub_count + [row_spec],
                [jax.ShapeDtypeStruct((count, chunk, LANES), f32)] * sub_count
                + [jax.ShapeDtypeStruct((count * GROUP, edge, LANES), f32)],
                [shifted, flat],
                count,
                flops * count // groups,
            )
            moved[start] = outs[sub_count]
            pieces += exchange(outs[:sub_count], "sub")
        outward = pieced
        solved = call(
            functools.partial(solve_kernel, sizes, sub_count, inward, outward),
            scalars,
            (*pieces, columns, own_levels, stacked),
            tall_specs(inward)
            + [whole(columns.shape), whole(own_levels.shape), whole(stacked.shape)],
            tall_specs(outward),
            [
                jax.ShapeDtypeStruct((count, chunk, LANES), f32)
                for _, count in outward
                for _ in range(sub_count)
            ],
            [pltpu.VMEM((tall // GROUP // 2, edge, 2 * LANES), f32)],
            solve_steps,
            flops,
        )
        received = [
            exchange(solved[part * sub_count : (part + 1) * sub_count], "sub")
            for part in range(len(outward))
        ]
        for part, (start, count) in enumerate(outward):
            origin = max(first for first in moved if first <= start)
            first, second = call(
                functools.partial(backward_kernel, sizes, sub_count, pad, slot),
                scalars,
                (*received[part], boxes, moved[origin], padded, stacked),
                [piece_spec] * sub_count
                + [
                    side(slot, 0, start),
                    rows_from(start - origin),
                    whole(padded.shape),
                    whole(stacked.shape),
                ],
                [row_spec, dense_spec],
                [
                    jax.ShapeDtypeStruct((count * GROUP, edge, LANES), f32),
                    jax.ShapeDtypeStruct((edge, count * lanes), f32),
                ],
                [shifted, flat],
                count,
                flops * count // groups,
            )
            firsts.append((slot, start, count, first))
            seconds.append((slot, start, count, second))
            returns.append((slot, start, count, from_behind(second, "slab", 1)))

    def group_spec(shape, axis, start, count):
        def index(g, *s):
            at = [0] * len(shape)
            at[axis] = jnp.clip(g - start, 0, count - 1)
            return tuple(at)

        return pl.BlockSpec(shape, index)

    early = [r for r in returns if r[0] < slot_count - 1]
    late = [r for r in returns if r[0] == slot_count - 1]
    layout = [
        [(slot, start) for slot, start, _, _ in pieces] for pieces in (firsts, seconds, early)
    ]
    edge_block = (orbital_count, 1, edge, LANES)
    partial = call(
        functools.partial(combine_kernel, sizes, layout),
        (*scalars, asked),
        (
            boxes,
            boxes,
            boxes,
            low_halo,
            high_halo,
            *(piece for pieces in (firsts, seconds, early) for *_, piece in pieces),
        ),
        [
            pl.BlockSpec((orbital_count, GROUP, edge, LANES), lambda g, *s: (0, g, 0, 0)),
            pl.BlockSpec(edge_block, lambda g, *s: (0, jnp.maximum(g * GROUP - 1, 0), 0, 0)),
            pl.BlockSpec(
                edge_block, lambda g, *s: (0, jnp.minimum((g + 1) * GROUP, rows - 1), 0, 0)
            ),
            whole((orbital_count, edge, LANES)),
            whole((orbital_count, edge, LANES)),
        ]
        + [group_spec((GROUP, edge, LANES), 0, start, count) for _, start, count, _ in firsts]
        + [
            group_spec((edge, lanes), 1, start, count)
            for pieces in (seconds, early)
            for _, start, count, _ in pieces
        ],
        [pl.BlockSpec((orbital_count, edge, lanes), lambda g, *s: (0, 0, g))],
        [jax.ShapeDtypeStruct(orbitals.shape, f32)],
        [pltpu.VMEM((2, edge + 2 * GROUP, LANES), f32)],
        groups,
        flops,
    )[0]
    partial = call(
        functools.partial(field_kernel, sizes, len(fields), folds),
        (corners, ids),
        (partial, boxes, *fields),
        [own_spec, pl.BlockSpec((orbital_count, GROUP, edge, LANES), lambda g, *s: (0, g, 0, 0))]
        + [
            pl.BlockSpec((f.shape[0], GROUP, plane_count, LANES), lambda g, *s: (0, g, 0, 0))
            for f in fields
        ],
        [own_spec],
        [jax.ShapeDtypeStruct(orbitals.shape, f32)],
        [pltpu.VMEM((GROUP, REACH * plane_count, LANES), f32)],
        groups,
        flops,
    )[0]

    slot, last_start, last_count, last_piece = late[-1]
    settled = partial
    if late[:-1]:
        settled = call(
            functools.partial(settle_kernel, slot, [start for _, start, *_ in late[:-1]], last_start),
            (asked, ids),
            (partial, *(piece for *_, piece in late[:-1])),
            [own_spec]
            + [group_spec((edge, lanes), 1, start, count) for _, start, count, _ in late[:-1]],
            [own_spec],
            [jax.ShapeDtypeStruct(orbitals.shape, f32)],
            [],
            groups,
            flops,
        )[0]

    def target(g, n, d):
        owned = n[slot, 1] - d[0] * orbital_count
        return (jnp.clip(owned, 0, orbital_count - 1), 0, g + last_start)

    target_spec = pl.BlockSpec((1, edge, lanes), target)
    return call(
        functools.partial(finish_kernel, orbital_count, slot),
        (asked, ids),
        (settled, partial, last_piece),
        [pl.BlockSpec(memory_space=pl.ANY), target_spec, dense_spec],
        [target_spec],
        [jax.ShapeDtypeStruct(orbitals.shape, f32)],
        [],
        last_count,
        flops,
        aliases={2: 0},
    )[0]


def solution(mesh):
    placed = (P("slab", None, "sub"), P("slab", "sub"), P(), P("slab", None), P("slab"))
    return jax.shard_map(
        program, mesh=mesh, in_specs=placed, out_specs=P("slab", None, "sub"), check_vma=False
    )
```
